768 devices in a mesh: seq: 64 (over y, x, core), head: 12 (over z).
Axes of the slice: x: 4, y: 8, z: 12, core: 2. Of those that a mesh axis runs over, the one named last changes fastest.
Arguments:
- query_raw: float32 [16384, 48, 128], P('seq', 'head'), may hold values from -150 to 150
- key_raw: float32 [16384, 48, 128], P('seq', 'head'), may hold values from -150 to 150
- value_raw: float32 [16384, 48, 128], P('seq', 'head'), may hold values from -6 to 6
- query_gain: float32 [48, 128], P('head'), may hold values from 0.25 to 1.75
- key_gain: float32 [48, 128], P('head'), may hold values from 0.25 to 1.75
- cotangent: float32 [16384, 48, 128], P('seq', 'head'), may hold values from -6 to 6
Outputs:
- attended: float32 [16384, 48, 128], P('seq', 'head')
- grad_query: float32 [16384, 48, 128], P('seq', 'head')
- grad_key: float32 [16384, 48, 128], P('seq', 'head')
- grad_value: float32 [16384, 48, 128], P('seq', 'head')
The draws below stay inside these ranges and needn't reach their ends.
All inputs are finite; a program needn't handle non-finite values.
Results may differ from the reference program's by a relative error of at most 0.00023.
Values sent between devices are 32-bit elements; how exact they have to be, the bound alone decides.
A program may use at most 64 MiB of HBM per device.

```python
import jax
import jax.numpy as jnp
from jax import lax

DK = 128
TOK_DEV = 256
HEADS = 48
TOKENS = 16384
N_SEQ = 64


def draw_scaled(key, salt):
    key = jax.random.fold_in(key, salt)
    first, second = jax.random.split(key, 2)
    channel = jnp.exp(jax.random.uniform(first, (HEADS, DK), jnp.float32) * jnp.log(10.0))
    ramp = jnp.exp(jnp.log(3.0) * jnp.arange(HEADS).astype(jnp.float32) / max(HEADS - 1, 1))
    base = jnp.clip(jax.random.normal(second, (TOKENS, HEADS, DK), jnp.float32), -5.0, 5.0)
    return (base * channel[None] * ramp[None, :, None]).astype(jnp.float32)


def draw_query_raw(key, part):
    return draw_scaled(key, 11)


def draw_key_raw(key, part):
    return draw_scaled(key, 23)


def shard_levels(key, shape, cuts, least, top_value):
    loudness, own = 1.0, jax.random.fold_in(key, 6)
    for axis_at, blocks in cuts:
        heights = jnp.exp(jax.random.uniform(jax.random.fold_in(own, axis_at), (blocks,), jnp.float32, least / len(cuts), top_value / len(cuts)))
        loudness = loudness * jnp.repeat(heights, shape[axis_at] // blocks).reshape([-1 if axis == axis_at else 1 for axis in range(len(shape))])
    return loudness


def centred(rng, dims, spread, limit, cuts=(), held_as=jnp.bfloat16):
    drawn = spread * jax.random.normal(rng, dims, jnp.float32)
    if cuts:
        drawn = drawn * shard_levels(rng, dims, cuts, -0.22, 0.18)
    return jnp.clip(drawn, -limit, limit).astype(held_as)


def setup_inputs(seed: int = 0) -> dict:
    seeds = jax.random.split(jax.random.key(seed), 7)
    return {
        "query_raw": draw_query_raw(jax.random.fold_in(seeds[6], 71), 0),
        "key_raw": draw_key_raw(jax.random.fold_in(seeds[6], 71), 0),
        "value_raw": centred(seeds[2], (TOKENS, HEADS, DK), 1.0, 6.0, ((0, 64), (1, 12)), jnp.float32),
        "query_gain": jnp.clip(1.0 + 0.15 * jax.random.normal(seeds[3], (HEADS, DK), jnp.float32), 0.25, 1.75),
        "key_gain": jnp.clip(1.0 + 0.15 * jax.random.normal(seeds[4], (HEADS, DK), jnp.float32), 0.25, 1.75),
        "cotangent": centred(seeds[5], (TOKENS, HEADS, DK), 1.0, 6.0, ((0, 64), (1, 12)), jnp.float32),
    }


epsilon = 1e-06
highest = lax.Precision.HIGHEST

def product(form, left, right):
    return jnp.einsum(form, left, right, precision=highest)

def normalize(raw, gain):
    scale = lax.rsqrt(lax.optimization_barrier(jnp.mean(raw * raw, axis=(1, 2), keepdims=True)) + epsilon)
    return raw * scale * gain[None]

def layer(query_in, key_in, value_in, query_gain, key_gain):
    query_hat = normalize(query_in, query_gain)
    key_hat = normalize(key_in, key_gain)
    query_blocks = query_hat.reshape(N_SEQ, TOK_DEV, HEADS, DK)
    key_blocks = key_hat.reshape(N_SEQ, TOK_DEV, HEADS, DK)
    value_blocks = value_in.reshape(N_SEQ, TOK_DEV, HEADS, DK)
    indices = jnp.arange(TOK_DEV)
    causal = indices[:, None] >= indices[None, :]

    def advance(state, blocks):
        query_blk, key_blk, value_blk = blocks
        scores = jnp.where(causal[None], product('thd,shd->hts', query_blk, key_blk), 0.0)
        result = product('hts,she->the', scores, value_blk) + product('thd,hde->the', query_blk, state)
        state = state + product('thd,the->hde', key_blk, value_blk)
        return (state, result)
    initial = jnp.zeros((HEADS, DK, DK), jnp.float32)
    _, outputs = lax.scan(jax.checkpoint(advance), initial, (query_blocks, key_blocks, value_blocks))
    position = jnp.arange(TOKENS).astype(jnp.float32)
    weight = lax.rsqrt(DK * (position + 1.0))
    return outputs.reshape(TOKENS, HEADS, DK) * weight[:, None, None]

def reference(query_raw, key_raw, value_raw, query_gain, key_gain, cotangent):

    def forward_only(query_in, key_in, value_in):
        return layer(query_in, key_in, value_in, query_gain, key_gain)
    attended, pullback = jax.vjp(forward_only, query_raw, key_raw, value_raw)
    grad_query, grad_key, grad_value = pullback(cotangent)
    return (attended, grad_query, grad_key, grad_value)
```

```python
import functools

import jax
import jax.numpy as jnp
from jax import lax
from jax.experimental import pallas as pl
from jax.experimental.pallas import tpu as pltpu
from jax.sharding import PartitionSpec as P

MESH = pl.DeviceIdType.MESH
EPSILON = 1e-06
F32, BF16 = jnp.float32, jnp.bfloat16

NN = ((1,), (0,))
NT = ((1,), (1,))
TN = ((0,), (0,))


def halves(x):
    high = x.astype(BF16)
    return high, (x - high.astype(F32)).astype(BF16)


def product(left, right, form):
    left_high, left_low = halves(left)
    right_high, right_low = halves(right)
    left_parts = jnp.concatenate([left_high, left_low, left_high], axis=form[0][0])
    right_parts = jnp.concatenate([right_high, right_high, right_low], axis=form[1][0])
    return lax.dot_general(left_parts, right_parts, (form, ((), ())), preferred_element_type=F32)


def lane_sums(x):
    high, low = halves(x)
    rest = (x - high.astype(F32) - low.astype(F32)).astype(BF16)
    parts = jnp.concatenate([high, low, rest], axis=1)
    ones = jnp.ones((8, parts.shape[1]), BF16)
    return lax.dot_general(ones, parts, (NT, ((), ())), preferred_element_type=F32)


def kernel(
    n_seq, n_head, heads, tokens, depth,
    q_hbm, k_hbm, v_hbm, c_hbm, q_gain, k_gain,
    att_ref, gq_ref, gk_ref, gv_ref,
    raw, unit, other, first, second, mix, score, weight, scales,
    z_send, z_recv, states, peer, chip_sum, gathered, prefixes, entering, passed, received,
    load_sem, z_sems, core_sems, scan_sems,
):
    chips = n_seq // 2
    share = heads * depth // chips
    seq, head = lax.axis_index("seq"), lax.axis_index("head")
    chip, core = seq // 2, seq % 2
    width = float(heads * n_head * depth)

    loads = [
        pltpu.make_async_copy(src, raw.at[i], load_sem.at[i])
        for i, src in enumerate((q_hbm, k_hbm, v_hbm, c_hbm))
    ]
    for load in loads:
        load.start()

    barrier = pltpu.get_barrier_semaphore()

    def greet_head(d, _):
        pl.semaphore_signal(
            barrier, inc=1, device_id=(seq, lax.rem(head + d, n_head)), device_id_type=MESH
        )
        return 0

    def greet_chip(d, _):
        to = lax.rem(chip + d, chips)
        pl.semaphore_signal(barrier, inc=1, device_id=(2 * to + core, head), device_id_type=MESH)
        return 0

    lax.fori_loop(1, n_head, greet_head, 0)
    lax.fori_loop(1, chips, greet_chip, 0)
    partner = (2 * chip + 1 - core, head)
    pl.semaphore_signal(barrier, inc=1, device_id=partner, device_id_type=MESH)

    def rows_of(h):
        return pl.ds(h, tokens, stride=heads)

    def share_sums(slot, of_query, of_key):
        send, recv = z_send.at[slot], z_recv.at[slot]
        for i, of_one in enumerate((of_query, of_key)):
            sums = lane_sums(of_one)
            for j in range(tokens // 128):
                send[pl.ds(2 * i + j, 1), :] = sums[0:1, 128 * j : 128 * (j + 1)]
        recv[head] = send[...]

    def share_copy(slot, d):
        return pltpu.make_async_remote_copy(
            src_ref=z_send.at[slot],
            dst_ref=z_recv.at[slot, head],
            send_sem=z_sems.at[2 * slot],
            recv_sem=z_sems.at[2 * slot + 1],
            device_id=(seq, lax.rem(head + d, n_head)),
            device_id_type=MESH,
        )

    def send_shares(slot):
        def body(i, _):
            step = (i + 1) // 2
            share_copy(slot, n_head // 2 + step * (1 - 2 * (i % 2))).start()
            return 0

        lax.fori_loop(0, n_head - 1, body, 0)

    def await_shares(slot):
        all_of = z_recv.at[slot, pl.ds(0, n_head - 1)]
        pltpu.make_async_copy(all_of, all_of, z_sems.at[2 * slot]).wait()
        pltpu.make_async_copy(all_of, all_of, z_sems.at[2 * slot + 1]).wait()
        return jnp.sum(z_recv[slot], axis=0)

    def down_rows(line, i):
        return jnp.concatenate(
            [
                jnp.broadcast_to(line[2 * i + j : 2 * i + j + 1, :], (128, 128)).T
                for j in range(tokens // 128)
            ],
            axis=0,
        )

    loads[0].wait()
    loads[1].wait()
    query_squares = jnp.zeros((tokens, depth), F32)
    key_squares = jnp.zeros((tokens, depth), F32)
    for h in range(heads):
        q, k = raw[0, rows_of(h), :], raw[1, rows_of(h), :]
        query_squares += q * q
        key_squares += k * k
    share_sums(0, query_squares, key_squares)

    pl.semaphore_wait(barrier, n_head - 1 + chips - 1 + 1)
    send_shares(0)

    loads[2].wait()
    loads[3].wait()
    position = (seq * tokens + lax.broadcasted_iota(jnp.int32, (tokens, depth), 0)).astype(F32)
    weight[...] = lax.rsqrt(float(depth) * (position + 1.0))
    for h in range(heads):
        other[0, h] = raw[3, rows_of(h), :] * weight[...]
        other[1, h] = raw[2, rows_of(h), :]

    rows = lax.broadcasted_iota(jnp.int32, (tokens, tokens), 0)
    columns = lax.broadcasted_iota(jnp.int32, (tokens, tokens), 1)
    causal = rows >= columns

    def mixing(h, _):
        mix[h] = jnp.where(causal, product(other[0, h], other[1, h], NT), 0.0)
        return 0

    lax.fori_loop(0, heads, mixing, 0)

    total = await_shares(0)
    scale = lax.rsqrt(total / width + EPSILON)
    for i in range(2):
        scales[i] = down_rows(scale, i)
    for i, gain in enumerate((q_gain, k_gain)):
        for h in range(heads):
            unit[i, h] = raw[i, rows_of(h), :] * scales[i] * gain[pl.ds(h, 1), :]

    def block_states(which):
        def body(h, _):
            at = pl.ds(pl.multiple_of(h * depth, depth), depth)
            states[which, at, :] = product(unit[1 - which, h], other[1 - which, h], TN)
            return 0

        lax.fori_loop(0, heads, body, 0)

    def to_partner(src, dst, i):
        return pltpu.make_async_remote_copy(
            src_ref=src,
            dst_ref=dst,
            send_sem=core_sems.at[2 * i],
            recv_sem=core_sems.at[2 * i + 1],
            device_id=partner,
            device_id_type=MESH,
        )

    block_states(1 - core)
    swap = to_partner(states.at[1 - core], peer, 0)
    swap.start()
    block_states(core)
    swap.wait()
    chip_sum[...] = states[core] + peer[...]

    def scan_rows(c):
        return pl.ds(pl.multiple_of(c * share, share), share)

    def scan_copy(src, dst, phase, to):
        return pltpu.make_async_remote_copy(
            src_ref=src,
            dst_ref=dst,
            send_sem=scan_sems.at[2 * phase],
            recv_sem=scan_sems.at[2 * phase + 1],
            device_id=(2 * to + core, head),
            device_id_type=MESH,
        )

    def scatter(i, _):
        to = lax.rem(chip + i, chips)
        scan_copy(chip_sum.at[scan_rows(to)], gathered.at[chip], 0, to).start()
        return 0

    def await_scan(phase):
        all_of = gathered.at[pl.ds(0, chips - 1)]
        pltpu.make_async_copy(all_of, all_of, scan_sems.at[2 * phase]).wait()
        pltpu.make_async_copy(all_of, all_of, scan_sems.at[2 * phase + 1]).wait()

    lax.fori_loop(1, chips, scatter, 0)
    gathered[chip] = chip_sum[scan_rows(chip), :]

    def scoring(h, _):
        score[h] = jnp.where(causal, product(unit[0, h], unit[1, h], NT), 0.0)
        return 0

    lax.fori_loop(0, heads, scoring, 0)
    await_scan(0)

    def prefix(i, running):
        c = i + core * (chips - 1 - 2 * i)
        prefixes[c] = running
        return running + gathered[c]

    lax.fori_loop(0, chips, prefix, jnp.zeros((share, depth), F32))

    def give_back(i, _):
        to = lax.rem(chip + i, chips)
        scan_copy(prefixes.at[to], entering.at[scan_rows(chip)], 1, to).start()
        return 0

    lax.fori_loop(1, chips, give_back, 0)
    entering[scan_rows(chip), :] = prefixes[chip]

    def inside(h, _):
        first[0, h] = product(score[h], other[1, h], NN)
        second[0, h] = product(mix[h], unit[1, h], NN)
        first[1, h] = product(score[h], other[0, h], TN)
        second[1, h] = product(mix[h], unit[0, h], TN)
        return 0

    lax.fori_loop(0, heads, inside, 0)
    await_scan(1)

    passed[...] = entering[...] + states[core]
    hand = to_partner(passed, received, 1)
    hand.start()

    def apply(which, state):
        def body(h, _):
            held = state[pl.ds(pl.multiple_of(h * depth, depth), depth), :]
            first[which, h] += product(unit[which, h], held, NN)
            second[which, h] += product(other[which, h], held, NT)
            return 0

        lax.fori_loop(0, heads, body, 0)

    apply(core, entering)
    hand.wait()
    apply(1 - core, received)

    query_inner = jnp.zeros((tokens, depth), F32)
    key_inner = jnp.zeros((tokens, depth), F32)
    for h in range(heads):
        query_inner += unit[0, h] * second[0, h]
        key_inner += unit[1, h] * second[1, h]
    share_sums(1, query_inner, key_inner)
    send_shares(1)
    for h in range(heads):
        att_ref[rows_of(h), :] = first[0, h] * weight[...]
        gv_ref[rows_of(h), :] = first[1, h]
    mean = await_shares(1) / width
    for i, (gain, out) in enumerate(((q_gain, gq_ref), (k_gain, gk_ref))):
        along = down_rows(mean, i) * scales[i]
        for h in range(heads):
            push = second[i, h] * gain[pl.ds(h, 1), :]
            out[rows_of(h), :] = scales[i] * (push - raw[i, rows_of(h), :] * along)


def local(n_seq, n_head, query_raw, key_raw, value_raw, query_gain, key_gain, cotangent):
    tokens, heads, depth = query_raw.shape
    chips = n_seq // 2
    flat = (tokens * heads, depth)
    states = (heads * depth, depth)
    per_owner = (chips, heads * depth // chips, depth)
    anywhere = pl.BlockSpec(memory_space=pl.ANY)
    vmem = pl.BlockSpec(memory_space=pltpu.VMEM)
    outs = pl.pallas_call(
        functools.partial(kernel, n_seq, n_head, heads, tokens, depth),
        out_shape=[jax.ShapeDtypeStruct(flat, F32)] * 4,
        in_specs=[anywhere] * 4 + [vmem] * 2,
        out_specs=[vmem] * 4,
        scratch_shapes=[
            pltpu.VMEM((4, *flat), F32),
            pltpu.VMEM((2, heads, tokens, depth), F32),
            pltpu.VMEM((2, heads, tokens, depth), F32),
            pltpu.VMEM((2, heads, tokens, depth), F32),
            pltpu.VMEM((2, heads, tokens, depth), F32),
            pltpu.VMEM((heads, tokens, tokens), F32),
            pltpu.VMEM((heads, tokens, tokens), F32),
            pltpu.VMEM((tokens, depth), F32),
            pltpu.VMEM((2, tokens, depth), F32),
            pltpu.VMEM((2, 2 * tokens // 128, 128), F32),
            pltpu.VMEM((2, n_head, 2 * tokens // 128, 128), F32),
            pltpu.VMEM((2, *states), F32),
            pltpu.VMEM(states, F32),
            pltpu.VMEM(states, F32),
            pltpu.VMEM(per_owner, F32),
            pltpu.VMEM(per_owner, F32),
            pltpu.VMEM(states, F32),
            pltpu.VMEM(states, F32),
            pltpu.VMEM(states, F32),
            pltpu.SemaphoreType.DMA((4,)),
            pltpu.SemaphoreType.DMA((4,)),
            pltpu.SemaphoreType.DMA((4,)),
            pltpu.SemaphoreType.DMA((4,)),
        ],
        compiler_params=pltpu.CompilerParams(
            collective_id=0, has_side_effects=True, vmem_limit_bytes=48 * 1024 * 1024
        ),
    )(
        *(x.reshape(flat) for x in (query_raw, key_raw, value_raw, cotangent)),
        query_gain,
        key_gain,
    )
    return tuple(x.reshape(tokens, heads, depth) for x in outs)


def solution(mesh):
    spec, gain = P("seq", "head", None), P("head", None)
    return jax.shard_map(
        functools.partial(local, mesh.shape["seq"], mesh.shape["head"]),
        mesh=mesh,
        in_specs=(spec, spec, spec, gain, gain, spec),
        out_specs=(spec,) * 4,
        check_vma=False,
    )
```

```python
import functools

import jax
import jax.numpy as jnp
from jax import lax
from jax.experimental import pallas as pl
from jax.experimental.pallas import tpu as pltpu
from jax.sharding import PartitionSpec as P

MESH = pl.DeviceIdType.MESH
EPSILON = 1e-06
CHIPS_X = 4
F32, BF16 = jnp.float32, jnp.bfloat16

NN = ((1,), (0,))
NT = ((1,), (1,))
TN = ((0,), (0,))


def halves(x):
    high = x.astype(BF16)
    return high, (x - high.astype(F32)).astype(BF16)


def product(left, right, form):
    left_high, left_low = halves(left)
    right_high, right_low = halves(right)
    left_parts = jnp.concatenate([left_high, left_low, left_high], axis=form[0][0])
    right_parts = jnp.concatenate([right_high, right_high, right_low], axis=form[1][0])
    return lax.dot_general(left_parts, right_parts, (form, ((), ())), preferred_element_type=F32)


def lane_sums(x):
    high, low = halves(x)
    rest = (x - high.astype(F32) - low.astype(F32)).astype(BF16)
    parts = jnp.concatenate([high, low, rest], axis=1)
    ones = jnp.ones((8, parts.shape[1]), BF16)
    return lax.dot_general(ones, parts, (NT, ((), ())), preferred_element_type=F32)


def kernel(
    n_seq, n_head, heads, tokens, depth,
    q_hbm, k_hbm, v_hbm, c_hbm, q_gain_hbm, k_gain_hbm,
    att_ref, gq_ref, gk_ref, gv_ref,
    raw, gains, unit, other, first, second, mix, score, weight, scales,
    z_send, z_recv, states, peer, chip_sum, gathered, prefixes, entering, passed, received,
    load_sem, z_sems, core_sems, scan_sems,
):
    chips = n_seq // 2
    share = heads * depth // chips
    seq, head = lax.axis_index("seq"), lax.axis_index("head")
    chip, core = seq // 2, seq % 2
    width = float(heads * n_head * depth)

    loads = [
        pltpu.make_async_copy(src, raw.at[i], load_sem.at[i])
        for i, src in enumerate((q_hbm, k_hbm, v_hbm, c_hbm))
    ] + [
        pltpu.make_async_copy(src, gains.at[i], load_sem.at[4 + i])
        for i, src in enumerate((q_gain_hbm, k_gain_hbm))
    ]
    for load in loads:
        load.start()

    barrier = pltpu.get_barrier_semaphore()

    def greet_head(d, _):
        pl.semaphore_signal(
            barrier, inc=1, device_id=(seq, lax.rem(head + d, n_head)), device_id_type=MESH
        )
        return 0

    def greet_chip(d, _):
        to = lax.rem(chip + d, chips)
        pl.semaphore_signal(barrier, inc=1, device_id=(2 * to + core, head), device_id_type=MESH)
        return 0

    lax.fori_loop(1, n_head, greet_head, 0)
    lax.fori_loop(1, chips, greet_chip, 0)
    partner = (2 * chip + 1 - core, head)
    pl.semaphore_signal(barrier, inc=1, device_id=partner, device_id_type=MESH)

    def rows_of(h):
        return pl.ds(h, tokens, stride=heads)

    def share_sums(slot, of_query, of_key):
        send, recv = z_send.at[slot], z_recv.at[slot]
        for i, of_one in enumerate((of_query, of_key)):
            sums = lane_sums(of_one)
            for j in range(tokens // 128):
                send[pl.ds(2 * i + j, 1), :] = sums[0:1, 128 * j : 128 * (j + 1)]
        recv[head] = send[...]

    def share_copy(slot, d):
        return pltpu.make_async_remote_copy(
            src_ref=z_send.at[slot],
            dst_ref=z_recv.at[slot, head],
            send_sem=z_sems.at[2 * slot],
            recv_sem=z_sems.at[2 * slot + 1],
            device_id=(seq, lax.rem(head + d, n_head)),
            device_id_type=MESH,
        )

    def send_shares(slot):
        def body(i, _):
            step = (i + 1) // 2
            share_copy(slot, n_head // 2 + step * (1 - 2 * (i % 2))).start()
            return 0

        lax.fori_loop(0, n_head - 1, body, 0)

    def await_shares(slot):
        all_of = z_recv.at[slot, pl.ds(0, n_head - 1)]
        pltpu.make_async_copy(all_of, all_of, z_sems.at[2 * slot]).wait()
        pltpu.make_async_copy(all_of, all_of, z_sems.at[2 * slot + 1]).wait()
        return jnp.sum(z_recv[slot], axis=0)

    def down_rows(line, i):
        return jnp.concatenate(
            [
                jnp.broadcast_to(line[2 * i + j : 2 * i + j + 1, :], (128, 128)).T
                for j in range(tokens // 128)
            ],
            axis=0,
        )

    loads[0].wait()
    loads[1].wait()
    query_squares = jnp.zeros((tokens, depth), F32)
    key_squares = jnp.zeros((tokens, depth), F32)
    for h in range(heads):
        q, k = raw[0, rows_of(h), :], raw[1, rows_of(h), :]
        query_squares += q * q
        key_squares += k * k
    share_sums(0, query_squares, key_squares)

    pl.semaphore_wait(barrier, n_head - 1 + chips - 1 + 1)
    send_shares(0)

    loads[2].wait()
    loads[3].wait()
    loads[4].wait()
    loads[5].wait()
    position = (seq * tokens + lax.broadcasted_iota(jnp.int32, (tokens, depth), 0)).astype(F32)
    weight[...] = lax.rsqrt(float(depth) * (position + 1.0))
    for h in range(heads):
        other[0, h] = raw[3, rows_of(h), :] * weight[...]
        other[1, h] = raw[2, rows_of(h), :]

    rows = lax.broadcasted_iota(jnp.int32, (tokens, tokens), 0)
    columns = lax.broadcasted_iota(jnp.int32, (tokens, tokens), 1)
    causal = rows >= columns

    def mixing(h, _):
        mix[h] = jnp.where(causal, product(other[0, h], other[1, h], NT), 0.0)
        return 0

    lax.fori_loop(0, heads, mixing, 0)

    total = await_shares(0)
    scale = lax.rsqrt(total / width + EPSILON)
    for i in range(2):
        scales[i] = down_rows(scale, i)
    for i in range(2):
        for h in range(heads):
            unit[i, h] = raw[i, rows_of(h), :] * scales[i] * gains[i, pl.ds(h, 1), :]

    def block_states(which):
        def body(h, _):
            at = pl.ds(pl.multiple_of(h * depth, depth), depth)
            states[which, at, :] = product(unit[1 - which, h], other[1 - which, h], TN)
            return 0

        lax.fori_loop(0, heads, body, 0)

    def to_partner(src, dst, i):
        return pltpu.make_async_remote_copy(
            src_ref=src,
            dst_ref=dst,
            send_sem=core_sems.at[2 * i],
            recv_sem=core_sems.at[2 * i + 1],
            device_id=partner,
            device_id_type=MESH,
        )

    block_states(1 - core)
    swap = to_partner(states.at[1 - core], peer, 0)
    swap.start()
    block_states(core)
    swap.wait()
    chip_sum[...] = states[core] + peer[...]

    def scan_rows(c):
        return pl.ds(pl.multiple_of(c * share, share), share)

    def scan_copy(src, dst, phase, to):
        return pltpu.make_async_remote_copy(
            src_ref=src,
            dst_ref=dst,
            send_sem=scan_sems.at[2 * phase],
            recv_sem=scan_sems.at[2 * phase + 1],
            device_id=(2 * to + core, head),
            device_id_type=MESH,
        )

    chips_x = min(CHIPS_X, chips)
    chips_y = chips // chips_x
    chip_y, chip_x = chip // chips_x, chip % chips_x
    steps = sorted(
        [(dy, dx) for dy in range(chips_y) for dx in range(chips_x) if dy or dx],
        key=lambda s: -(min(s[0], chips_y - s[0]) + min(s[1], chips_x - s[1])),
    )
    others = [
        lax.rem(chip_y + dy, chips_y) * chips_x + lax.rem(chip_x + dx, chips_x) for dy, dx in steps
    ]

    def await_scan(phase):
        all_of = gathered.at[pl.ds(0, chips - 1)]
        pltpu.make_async_copy(all_of, all_of, scan_sems.at[2 * phase]).wait()
        pltpu.make_async_copy(all_of, all_of, scan_sems.at[2 * phase + 1]).wait()

    for to in others:
        scan_copy(chip_sum.at[scan_rows(to)], gathered.at[chip], 0, to).start()
    gathered[chip] = chip_sum[scan_rows(chip), :]

    def scoring(h, _):
        score[h] = jnp.where(causal, product(unit[0, h], unit[1, h], NT), 0.0)
        return 0

    lax.fori_loop(0, heads, scoring, 0)
    await_scan(0)

    running = jnp.zeros((share, depth), F32)
    for i in range(chips):
        c = i + core * (chips - 1 - 2 * i)
        prefixes[c] = running
        running = running + gathered[c]

    for to in others:
        scan_copy(prefixes.at[to], entering.at[scan_rows(chip)], 1, to).start()
    entering[scan_rows(chip), :] = prefixes[chip]

    def inside(h, _):
        first[0, h] = product(score[h], other[1, h], NN)
        second[0, h] = product(mix[h], unit[1, h], NN)
        first[1, h] = product(score[h], other[0, h], TN)
        second[1, h] = product(mix[h], unit[0, h], TN)
        return 0

    lax.fori_loop(0, heads, inside, 0)
    await_scan(1)

    passed[...] = entering[...] + states[core]
    hand = to_partner(passed, received, 1)
    hand.start()

    def each_state(state, body):
        def at_head(h, _):
            body(h, state[pl.ds(pl.multiple_of(h * depth, depth), depth), :])
            return 0

        lax.fori_loop(0, heads, at_head, 0)

    def apply_second(which, state):
        def body(h, held):
            second[which, h] += product(other[which, h], held, NT)

        each_state(state, body)

    def apply_first(which, state):
        def body(h, held):
            first[which, h] += product(unit[which, h], held, NN)

        each_state(state, body)

    apply_second(core, entering)
    hand.wait()
    apply_second(1 - core, received)

    inner = [jnp.zeros((tokens, depth), F32) for _ in range(2)]
    for h in range(heads):
        for i in range(2):
            inner[i] += unit[i, h] * second[i, h]
    share_sums(1, *inner)
    send_shares(1)

    apply_first(core, entering)
    apply_first(1 - core, received)
    for h in range(heads):
        att_ref[rows_of(h), :] = first[0, h] * weight[...]
        gv_ref[rows_of(h), :] = first[1, h]
    for i in range(2):
        for h in range(heads):
            second[i, h] = second[i, h] * gains[i, pl.ds(h, 1), :] * scales[i]
            other[i, h] = raw[i, rows_of(h), :] * (scales[i] * scales[i])
    mean = await_shares(1) / width
    for i, out in enumerate((gq_ref, gk_ref)):
        along = down_rows(mean, i)
        for h in range(heads):
            out[rows_of(h), :] = second[i, h] - other[i, h] * along


def leave(*refs):
    sources, targets, sems = refs[:4], refs[4:8], refs[8]
    copies = [
        pltpu.make_async_copy(src, dst, sems.at[i])
        for i, (src, dst) in enumerate(zip(sources, targets))
    ]
    for copy in copies:
        copy.start()
    for copy in copies:
        copy.wait()


def kept(x):
    return pltpu.with_memory_space_constraint(x, pltpu.HBM)


def local(n_seq, n_head, query_raw, key_raw, value_raw, query_gain, key_gain, cotangent):
    tokens, heads, depth = query_raw.shape
    chips = n_seq // 2
    flat = (tokens * heads, depth)
    states = (heads * depth, depth)
    per_owner = (chips, heads * depth // chips, depth)
    hbm = pl.BlockSpec(memory_space=pltpu.HBM)
    vmem = pl.BlockSpec(memory_space=pltpu.VMEM)
    outs = pl.pallas_call(
        functools.partial(kernel, n_seq, n_head, heads, tokens, depth),
        out_shape=[jax.ShapeDtypeStruct(flat, F32)] * 4,
        in_specs=[hbm] * 6,
        out_specs=[vmem] * 4,
        scratch_shapes=[
            pltpu.VMEM((4, *flat), F32),
            pltpu.VMEM((2, heads, depth), F32),
            pltpu.VMEM((2, heads, tokens, depth), F32),
            pltpu.VMEM((2, heads, tokens, depth), F32),
            pltpu.VMEM((2, heads, tokens, depth), F32),
            pltpu.VMEM((2, heads, tokens, depth), F32),
            pltpu.VMEM((heads, tokens, tokens), F32),
            pltpu.VMEM((heads, tokens, tokens), F32),
            pltpu.VMEM((tokens, depth), F32),
            pltpu.VMEM((2, tokens, depth), F32),
            pltpu.VMEM((2, 2 * tokens // 128, 128), F32),
            pltpu.VMEM((2, n_head, 2 * tokens // 128, 128), F32),
            pltpu.VMEM((2, *states), F32),
            pltpu.VMEM(states, F32),
            pltpu.VMEM(states, F32),
            pltpu.VMEM(per_owner, F32),
            pltpu.VMEM(per_owner, F32),
            pltpu.VMEM(states, F32),
            pltpu.VMEM(states, F32),
            pltpu.VMEM(states, F32),
            pltpu.SemaphoreType.DMA((6,)),
            pltpu.SemaphoreType.DMA((4,)),
            pltpu.SemaphoreType.DMA((4,)),
            pltpu.SemaphoreType.DMA((4,)),
        ],
        compiler_params=pltpu.CompilerParams(
            collective_id=0, has_side_effects=True, vmem_limit_bytes=48 * 1024 * 1024
        ),
    )(
        *(kept(x.reshape(flat)) for x in (query_raw, key_raw, value_raw, cotangent)),
        kept(query_gain),
        kept(key_gain),
    )
    outs = pl.pallas_call(
        leave,
        out_shape=[jax.ShapeDtypeStruct(flat, F32)] * 4,
        in_specs=[vmem] * 4,
        out_specs=[hbm] * 4,
        scratch_shapes=[pltpu.SemaphoreType.DMA((4,))],
        compiler_params=pltpu.CompilerParams(vmem_limit_bytes=4 * 1024 * 1024),
    )(*outs)
    return tuple(x.reshape(tokens, heads, depth) for x in outs)


def solution(mesh):
    spec, gain = P("seq", "head", None), P("head", None)
    return jax.shard_map(
        functools.partial(local, mesh.shape["seq"], mesh.shape["head"]),
        mesh=mesh,
        in_specs=(spec, spec, spec, gain, gain, spec),
        out_specs=(spec,) * 4,
        check_vma=False,
    )
```

```python
import functools

import jax
import jax.numpy as jnp
from jax import lax
from jax.experimental import pallas as pl
from jax.experimental.pallas import tpu as pltpu
from jax.sharding import PartitionSpec as P

MESH = pl.DeviceIdType.MESH
EPSILON = 1e-06
CHIPS_X = 4
F32, BF16 = jnp.float32, jnp.bfloat16

NN = ((1,), (0,))
NT = ((1,), (1,))
TN = ((0,), (0,))


def halves(x):
    high = x.astype(BF16)
    return high, (x - high.astype(F32)).astype(BF16)


def left_parts(x, axis):
    high, low = halves(x)
    return jnp.concatenate([high, low, high], axis=axis)


def right_parts(x, axis):
    high, low = halves(x)
    return jnp.concatenate([high, high, low], axis=axis)


def dot(left, right, form):
    return lax.dot_general(left, right, (form, ((), ())), preferred_element_type=F32)


def product(left, right, form):
    return dot(left_parts(left, form[0][0]), right_parts(right, form[1][0]), form)


def lane_sums(x):
    high, low = halves(x)
    rest = (x - high.astype(F32) - low.astype(F32)).astype(BF16)
    parts = jnp.concatenate([high, low, rest], axis=1)
    ones = jnp.ones((8, parts.shape[1]), BF16)
    return dot(ones, parts, NT)


def down_rows(line, i, tokens):
    return jnp.concatenate(
        [
            jnp.broadcast_to(line[2 * i + j : 2 * i + j + 1, :], (128, 128)).T
            for j in range(tokens // 128)
        ],
        axis=0,
    )


def kernel(
    n_seq, n_head, heads, tokens, depth,
    q_hbm, k_hbm, v_hbm, c_hbm, q_gain_hbm, k_gain_hbm,
    att_ref, gv_ref, push_ref, base_ref, mean_ref,
    raw, gains, unit, other, turned, split, first, second, mix, score, weight, scales,
    z_send, z_recv, states, peer, chip_sum, gathered, prefixes, entering, passed, received,
    load_sem, z_sems, core_sems, scan_sems,
):
    chips = n_seq // 2
    share = heads * depth // chips
    seq, head = lax.axis_index("seq"), lax.axis_index("head")
    chip, core = seq // 2, seq % 2
    width = float(heads * n_head * depth)

    loads = [
        pltpu.make_async_copy(src, raw.at[i], load_sem.at[i])
        for i, src in enumerate((q_hbm, k_hbm, v_hbm, c_hbm))
    ] + [
        pltpu.make_async_copy(src, gains.at[i], load_sem.at[4 + i])
        for i, src in enumerate((q_gain_hbm, k_gain_hbm))
    ]
    for load in loads:
        load.start()

    barrier = pltpu.get_barrier_semaphore()

    def greet_head(d, _):
        pl.semaphore_signal(
            barrier, inc=1, device_id=(seq, lax.rem(head + d, n_head)), device_id_type=MESH
        )
        return 0

    def greet_chip(d, _):
        to = lax.rem(chip + d, chips)
        pl.semaphore_signal(barrier, inc=1, device_id=(2 * to + core, head), device_id_type=MESH)
        return 0

    lax.fori_loop(1, n_head, greet_head, 0)
    lax.fori_loop(1, chips, greet_chip, 0)
    partner = (2 * chip + 1 - core, head)
    pl.semaphore_signal(barrier, inc=1, device_id=partner, device_id_type=MESH)

    def rows_of(h):
        return pl.ds(h, tokens, stride=heads)

    def share_sums(slot, of_query, of_key):
        send, recv = z_send.at[slot], z_recv.at[slot]
        for i, of_one in enumerate((of_query, of_key)):
            sums = lane_sums(of_one)
            for j in range(tokens // 128):
                send[pl.ds(2 * i + j, 1), :] = sums[0:1, 128 * j : 128 * (j + 1)]
        recv[head] = send[...]

    def share_copy(slot, d):
        return pltpu.make_async_remote_copy(
            src_ref=z_send.at[slot],
            dst_ref=z_recv.at[slot, head],
            send_sem=z_sems.at[2 * slot],
            recv_sem=z_sems.at[2 * slot + 1],
            device_id=(seq, lax.rem(head + d, n_head)),
            device_id_type=MESH,
        )

    def send_shares(slot):
        def body(i, _):
            step = (i + 1) // 2
            share_copy(slot, n_head // 2 + step * (1 - 2 * (i % 2))).start()
            return 0

        lax.fori_loop(0, n_head - 1, body, 0)

    def await_shares(slot):
        all_of = z_recv.at[slot, pl.ds(0, n_head - 1)]
        pltpu.make_async_copy(all_of, all_of, z_sems.at[2 * slot + 1]).wait()
        return jnp.sum(z_recv[slot], axis=0)

    loads[0].wait()
    loads[1].wait()
    query_squares = jnp.zeros((tokens, depth), F32)
    key_squares = jnp.zeros((tokens, depth), F32)
    for h in range(heads):
        q, k = raw[0, rows_of(h), :], raw[1, rows_of(h), :]
        query_squares += q * q
        key_squares += k * k
    share_sums(0, query_squares, key_squares)

    pl.semaphore_wait(barrier, n_head - 1 + chips - 1 + 1)
    send_shares(0)

    loads[2].wait()
    loads[3].wait()
    loads[4].wait()
    loads[5].wait()
    position = (seq * tokens + lax.broadcasted_iota(jnp.int32, (tokens, depth), 0)).astype(F32)
    weight[...] = lax.rsqrt(float(depth) * (position + 1.0))
    for h in range(heads):
        other[0, h] = raw[3, rows_of(h), :] * weight[...]
        other[1, h] = raw[2, rows_of(h), :]
    for i in range(2):
        for h in range(heads):
            unit[i, h] = raw[i, rows_of(h), :] * gains[i, pl.ds(h, 1), :]

    def turning(h, _):
        for i in range(2):
            turned[i, h] = left_parts(other[i, h].T, 1)
            split[i, h] = left_parts(other[i, h], 1)
        return 0

    lax.fori_loop(0, heads, turning, 0)

    rows = lax.broadcasted_iota(jnp.int32, (tokens, tokens), 0)
    columns = lax.broadcasted_iota(jnp.int32, (tokens, tokens), 1)
    causal = rows >= columns

    def mixing(h, _):
        mix[h] = jnp.where(causal, product(other[0, h], other[1, h], NT), 0.0)
        return 0

    lax.fori_loop(0, heads, mixing, 0)

    total = await_shares(0)
    scale = lax.rsqrt(total / width + EPSILON)
    for i in range(2):
        scales[i] = down_rows(scale, i, tokens)

    def at_head(h):
        return pl.ds(h * depth, depth)

    def block_state(which, h):
        normed = unit[1 - which, h] * scales[1 - which]
        unit[1 - which, h] = normed
        states[which, at_head(h), :] = dot(turned[1 - which, h], right_parts(normed, 0), NN)

    def to_partner(src, dst, phase, h):
        return pltpu.make_async_remote_copy(
            src_ref=src.at[at_head(h)],
            dst_ref=dst.at[at_head(h)],
            send_sem=core_sems.at[phase, 0, h],
            recv_sem=core_sems.at[phase, 1, h],
            device_id=partner,
            device_id_type=MESH,
        )

    swaps = [to_partner(states.at[1 - core], peer, 0, h) for h in range(heads)]
    for h in range(heads):
        block_state(1 - core, h)
        swaps[h].start()
    for h in range(heads):
        block_state(core, h)
    for h in range(heads):
        swaps[h].wait_recv()
        chip_sum[at_head(h), :] = states[core, at_head(h), :] + peer[at_head(h), :]

    def scan_rows(c):
        return pl.ds(pl.multiple_of(c * share, share), share)

    def scan_copy(src, dst, phase, to):
        return pltpu.make_async_remote_copy(
            src_ref=src,
            dst_ref=dst,
            send_sem=scan_sems.at[2 * phase],
            recv_sem=scan_sems.at[2 * phase + 1],
            device_id=(2 * to + core, head),
            device_id_type=MESH,
        )

    chips_x = min(CHIPS_X, chips)
    chips_y = chips // chips_x
    chip_y, chip_x = chip // chips_x, chip % chips_x
    steps = sorted(
        [(dy, dx) for dy in range(chips_y) for dx in range(chips_x) if dy or dx],
        key=lambda s: -(min(s[0], chips_y - s[0]) + min(s[1], chips_x - s[1])),
    )
    others = [
        lax.rem(chip_y + dy, chips_y) * chips_x + lax.rem(chip_x + dx, chips_x) for dy, dx in steps
    ]

    def await_scan(phase):
        all_of = gathered.at[pl.ds(0, chips - 1)]
        pltpu.make_async_copy(all_of, all_of, scan_sems.at[2 * phase + 1]).wait()

    for to in others:
        scan_copy(chip_sum.at[scan_rows(to)], gathered.at[chip], 0, to).start()
    gathered[chip] = chip_sum[scan_rows(chip), :]

    def scoring(h, _):
        score[h] = jnp.where(causal, product(unit[0, h], unit[1, h], NT), 0.0)
        return 0

    lax.fori_loop(0, heads, scoring, 0)
    await_scan(0)

    running = jnp.zeros((share, depth), F32)
    for i in range(chips):
        c = i + core * (chips - 1 - 2 * i)
        prefixes[c] = running
        running = running + gathered[c]

    for to in others:
        scan_copy(prefixes.at[to], entering.at[scan_rows(chip)], 1, to).start()
    entering[scan_rows(chip), :] = prefixes[chip]

    def inside(h, _):
        first[0, h] = product(score[h], other[1, h], NN)
        second[0, h] = product(mix[h], unit[1, h], NN)
        first[1, h] = product(score[h], other[0, h], TN)
        second[1, h] = product(mix[h], unit[0, h], TN)
        return 0

    lax.fori_loop(0, heads, inside, 0)
    await_scan(1)

    hands = [to_partner(passed, received, 1, h) for h in range(heads)]
    for h in range(heads):
        passed[at_head(h), :] = entering[at_head(h), :] + states[core, at_head(h), :]
        hands[h].start()

    def apply_second(which, state, h):
        second[which, h] += dot(split[which, h], right_parts(state[at_head(h), :], 0), NN)

    def apply_first(which, state):
        def body(h, _):
            held = state[pl.ds(pl.multiple_of(h * depth, depth), depth), :]
            first[which, h] += product(unit[which, h], held, NT)
            return 0

        lax.fori_loop(0, heads, body, 0)

    for h in range(heads):
        apply_second(core, entering, h)
    for h in range(heads):
        hands[h].wait_recv()
        apply_second(1 - core, received, h)

    inner = [jnp.zeros((tokens, depth), F32) for _ in range(2)]
    for h in range(heads):
        for i in range(2):
            inner[i] += unit[i, h] * second[i, h]
    share_sums(1, *inner)
    send_shares(1)

    apply_first(core, entering)
    apply_first(1 - core, received)
    for h in range(heads):
        att_ref[rows_of(h), :] = first[0, h] * weight[...]
        gv_ref[rows_of(h), :] = first[1, h]
    for i in range(2):
        for h in range(heads):
            push_ref[i, h] = second[i, h] * gains[i, pl.ds(h, 1), :] * scales[i]
            base_ref[i, h] = raw[i, rows_of(h), :] * (scales[i] * scales[i])
    mean_ref[...] = await_shares(1) / width

    for h in range(heads):
        swaps[h].wait_send()
        hands[h].wait_send()
    for slot in range(2):
        all_of = z_recv.at[slot, pl.ds(0, n_head - 1)]
        pltpu.make_async_copy(all_of, all_of, z_sems.at[2 * slot]).wait()
    for phase in range(2):
        all_of = gathered.at[pl.ds(0, chips - 1)]
        pltpu.make_async_copy(all_of, all_of, scan_sems.at[2 * phase]).wait()


def leave(
    heads, tokens, att_ref, gv_ref, push_ref, base_ref, mean_ref,
    att_out, gq_out, gk_out, gv_out, staged, sems,
):
    copies = [
        pltpu.make_async_copy(src, dst, sems.at[i])
        for i, (src, dst) in enumerate(
            ((att_ref, att_out), (gv_ref, gv_out), (staged.at[0], gq_out), (staged.at[1], gk_out))
        )
    ]
    copies[0].start()
    copies[1].start()
    mean = mean_ref[...]
    for i in range(2):
        along = down_rows(mean, i, tokens)
        for h in range(heads):
            rows = pl.ds(h, tokens, stride=heads)
            staged[i, rows, :] = push_ref[i, h] - base_ref[i, h] * along
        copies[2 + i].start()
    for copy in copies:
        copy.wait()


def kept(x):
    return pltpu.with_memory_space_constraint(x, pltpu.HBM)


def local(n_seq, n_head, query_raw, key_raw, value_raw, query_gain, key_gain, cotangent):
    tokens, heads, depth = query_raw.shape
    chips = n_seq // 2
    flat = (tokens * heads, depth)
    both = (2, heads, tokens, depth)
    states = (heads * depth, depth)
    per_owner = (chips, heads * depth // chips, depth)
    hbm = pl.BlockSpec(memory_space=pltpu.HBM)
    vmem = pl.BlockSpec(memory_space=pltpu.VMEM)
    outs = pl.pallas_call(
        functools.partial(kernel, n_seq, n_head, heads, tokens, depth),
        out_shape=[
            jax.ShapeDtypeStruct(shape, F32)
            for shape in (flat, flat, both, both, (2 * tokens // 128, 128))
        ],
        in_specs=[hbm] * 6,
        out_specs=[vmem] * 5,
        scratch_shapes=[
            pltpu.VMEM((4, *flat), F32),
            pltpu.VMEM((2, heads, depth), F32),
            pltpu.VMEM(both, F32),
            pltpu.VMEM(both, F32),
            pltpu.VMEM((2, heads, depth, 3 * tokens), BF16),
            pltpu.VMEM((2, heads, tokens, 3 * depth), BF16),
            pltpu.VMEM(both, F32),
            pltpu.VMEM(both, F32),
            pltpu.VMEM((heads, tokens, tokens), F32),
            pltpu.VMEM((heads, tokens, tokens), F32),
            pltpu.VMEM((tokens, depth), F32),
            pltpu.VMEM((2, tokens, depth), F32),
            pltpu.VMEM((2, 2 * tokens // 128, 128), F32),
            pltpu.VMEM((2, n_head, 2 * tokens // 128, 128), F32),
            pltpu.VMEM((2, *states), F32),
            pltpu.VMEM(states, F32),
            pltpu.VMEM(states, F32),
            pltpu.VMEM(per_owner, F32),
            pltpu.VMEM(per_owner, F32),
            pltpu.VMEM(states, F32),
            pltpu.VMEM(states, F32),
            pltpu.VMEM(states, F32),
            pltpu.SemaphoreType.DMA((6,)),
            pltpu.SemaphoreType.DMA((4,)),
            pltpu.SemaphoreType.DMA((2, 2, heads)),
            pltpu.SemaphoreType.DMA((4,)),
        ],
        compiler_params=pltpu.CompilerParams(
            collective_id=0, has_side_effects=True, vmem_limit_bytes=48 * 1024 * 1024
        ),
    )(
        *(kept(x.reshape(flat)) for x in (query_raw, key_raw, value_raw, cotangent)),
        kept(query_gain),
        kept(key_gain),
    )
    outs = pl.pallas_call(
        functools.partial(leave, heads, tokens),
        out_shape=[jax.ShapeDtypeStruct(flat, F32)] * 4,
        in_specs=[vmem] * 5,
        out_specs=[hbm] * 4,
        scratch_shapes=[pltpu.VMEM((2, *flat), F32), pltpu.SemaphoreType.DMA((4,))],
        compiler_params=pltpu.CompilerParams(vmem_limit_bytes=4 * 1024 * 1024),
    )(*outs)
    return tuple(x.reshape(tokens, heads, depth) for x in outs)


def solution(mesh):
    spec, gain = P("seq", "head", None), P("head", None)
    return jax.shard_map(
        functools.partial(local, mesh.shape["seq"], mesh.shape["head"]),
        mesh=mesh,
        in_specs=(spec, spec, spec, gain, gain, spec),
        out_specs=(spec,) * 4,
        check_vma=False,
    )
```

```python
import functools

import jax
import jax.numpy as jnp
from jax import lax
from jax.experimental import pallas as pl
from jax.experimental.pallas import tpu as pltpu
from jax.sharding import PartitionSpec as P

MESH = pl.DeviceIdType.MESH
EPSILON = 1e-06
CHIPS_X = 4
F32, BF16 = jnp.float32, jnp.bfloat16

NN = ((1,), (0,))
NT = ((1,), (1,))
TN = ((0,), (0,))


def halves(x):
    high = x.astype(BF16)
    return high, (x - high.astype(F32)).astype(BF16)


def left_parts(x, axis):
    high, low = halves(x)
    return jnp.concatenate([high, low, high], axis=axis)


def right_parts(x, axis):
    high, low = halves(x)
    return jnp.concatenate([high, high, low], axis=axis)


def dot(left, right, form):
    return lax.dot_general(left, right, (form, ((), ())), preferred_element_type=F32)


def product(left, right, form):
    return dot(left_parts(left, form[0][0]), right_parts(right, form[1][0]), form)


def lane_sums(x):
    high, low = halves(x)
    rest = (x - high.astype(F32) - low.astype(F32)).astype(BF16)
    parts = jnp.concatenate([high, low, rest], axis=1)
    ones = jnp.ones((8, parts.shape[1]), BF16)
    return dot(ones, parts, NT)


def down_rows(line, i, tokens):
    return jnp.concatenate(
        [
            jnp.broadcast_to(line[2 * i + j : 2 * i + j + 1, :], (128, 128)).T
            for j in range(tokens // 128)
        ],
        axis=0,
    )


def kernel(
    n_seq, n_head, heads, tokens, depth,
    q_hbm, k_hbm, v_hbm, c_hbm, q_gain_hbm, k_gain_hbm,
    att_ref, gv_ref, push_ref, base_ref, mean_ref,
    raw, gains, unit, other, turned, split, first, second, mix, score, weight, scales,
    z_send, z_recv, part_send, part_recv, line_scale, staged_unit, peer_unit, peer_other,
    peer_split,
    states, peer, chip_sum, gathered, prefixes, entering, passed, received,
    load_sem, z_sems, part_sems, push_sems, core_sems, scan_sems,
):
    chips = n_seq // 2
    share = heads * depth // chips
    seq, head = lax.axis_index("seq"), lax.axis_index("head")
    chip, core = seq // 2, seq % 2
    width = float(heads * n_head * depth)

    loads = [
        pltpu.make_async_copy(src, raw.at[i], load_sem.at[i])
        for i, src in enumerate((q_hbm, k_hbm, v_hbm, c_hbm))
    ] + [
        pltpu.make_async_copy(src, gains.at[i], load_sem.at[4 + i])
        for i, src in enumerate((q_gain_hbm, k_gain_hbm))
    ]
    for load in loads:
        load.start()

    barrier = pltpu.get_barrier_semaphore()

    chips_x = min(CHIPS_X, chips)
    chips_y = chips // chips_x
    chip_y, chip_x = chip // chips_x, chip % chips_x
    steps = sorted(
        [(dy, dx) for dy in range(chips_y) for dx in range(chips_x) if dy or dx],
        key=lambda s: -(min(s[0], chips_y - s[0]) + min(s[1], chips_x - s[1])),
    )
    others = [
        lax.rem(chip_y + dy, chips_y) * chips_x + lax.rem(chip_x + dx, chips_x) for dy, dx in steps
    ]
    heads_on = [
        lax.rem(head + d, n_head)
        for d in sorted(range(1, n_head), key=lambda d: -min(d, n_head - d))
    ]
    peer_seq = 2 * chip + 1 - core
    partner = (peer_seq, head)
    greeted = [(seq, to) for to in heads_on] + [(2 * to + core, head) for to in others]
    greeted += [(peer_seq, to) for to in heads_on] + [partner]
    for device in greeted:
        pl.semaphore_signal(barrier, inc=1, device_id=device, device_id_type=MESH)

    def rows_of(h):
        return pl.ds(h, tokens, stride=heads)

    def share_sums(slot, of_query, of_key):
        send, recv = z_send.at[slot], z_recv.at[slot]
        for i, of_one in enumerate((of_query, of_key)):
            sums = lane_sums(of_one)
            for j in range(tokens // 128):
                send[pl.ds(2 * i + j, 1), :] = sums[0:1, 128 * j : 128 * (j + 1)]
        recv[head] = send[...]

    def share_copy(slot, to):
        return pltpu.make_async_remote_copy(
            src_ref=z_send.at[slot],
            dst_ref=z_recv.at[slot, head],
            send_sem=z_sems.at[2 * slot],
            recv_sem=z_sems.at[2 * slot + 1],
            device_id=(seq, to),
            device_id_type=MESH,
        )

    def send_shares(slot):
        for to in heads_on:
            share_copy(slot, to).start()

    def part_copy(kind, device):
        return pltpu.make_async_remote_copy(
            src_ref=part_send.at[kind],
            dst_ref=part_recv.at[kind, head],
            send_sem=part_sems.at[2 * kind],
            recv_sem=part_sems.at[2 * kind + 1],
            device_id=device,
            device_id_type=MESH,
        )

    def await_shares(slot):
        all_of = z_recv.at[slot, pl.ds(0, n_head - 1)]
        pltpu.make_async_copy(all_of, all_of, z_sems.at[2 * slot + 1]).wait()
        return jnp.sum(z_recv[slot], axis=0)

    loads[0].wait()
    loads[1].wait()
    query_squares = jnp.zeros((tokens, depth), F32)
    key_squares = jnp.zeros((tokens, depth), F32)
    for h in range(heads):
        q, k = raw[0, rows_of(h), :], raw[1, rows_of(h), :]
        query_squares += q * q
        key_squares += k * k
    share_sums(0, query_squares, key_squares)

    pl.semaphore_wait(barrier, len(greeted))
    send_shares(0)

    loads[2].wait()
    loads[3].wait()
    loads[4].wait()
    loads[5].wait()
    position = (seq * tokens + lax.broadcasted_iota(jnp.int32, (tokens, depth), 0)).astype(F32)
    weight[...] = lax.rsqrt(float(depth) * (position + 1.0))
    for h in range(heads):
        other[0, h] = raw[3, rows_of(h), :] * weight[...]
        other[1, h] = raw[2, rows_of(h), :]
    for i in range(2):
        for h in range(heads):
            unit[i, h] = raw[i, rows_of(h), :] * gains[i, pl.ds(h, 1), :]

    pushes = [
        pltpu.make_async_remote_copy(
            src_ref=src,
            dst_ref=dst,
            send_sem=push_sems.at[2 * i],
            recv_sem=push_sems.at[2 * i + 1],
            device_id=partner,
            device_id_type=MESH,
        )
        for i, (src, dst) in enumerate(
            ((other.at[1 - core], peer_other), (staged_unit, peer_unit))
        )
    ]
    for h in range(heads):
        staged_unit[h] = unit[1 - core, h]
    for push in pushes:
        push.start()

    def turning(h, _):
        for i in range(2):
            turned[i, h] = left_parts(other[i, h].T, 1)
            split[i, h] = left_parts(other[i, h], 1)
        return 0

    lax.fori_loop(0, heads, turning, 0)

    rows = lax.broadcasted_iota(jnp.int32, (tokens, tokens), 0)
    columns = lax.broadcasted_iota(jnp.int32, (tokens, tokens), 1)
    causal = rows >= columns

    def mixing(h, _):
        mix[h] = jnp.where(causal, product(other[0, h], other[1, h], NT), 0.0)
        return 0

    lax.fori_loop(0, heads, mixing, 0)

    total = await_shares(0)
    scale = lax.rsqrt(total / width + EPSILON)
    line_scale[...] = scale
    for i in range(2):
        scales[i] = down_rows(scale, i, tokens)

    def at_head(h):
        return pl.ds(h * depth, depth)

    def block_state(which, h):
        normed = unit[1 - which, h] * scales[1 - which]
        unit[1 - which, h] = normed
        states[which, at_head(h), :] = dot(turned[1 - which, h], right_parts(normed, 0), NN)

    def to_partner(src, dst, phase, h):
        return pltpu.make_async_remote_copy(
            src_ref=src.at[at_head(h)],
            dst_ref=dst.at[at_head(h)],
            send_sem=core_sems.at[phase, 0, h],
            recv_sem=core_sems.at[phase, 1, h],
            device_id=partner,
            device_id_type=MESH,
        )

    swaps = [to_partner(states.at[1 - core], peer, 0, h) for h in range(heads)]
    for h in range(heads):
        block_state(1 - core, h)
        swaps[h].start()
    for h in range(heads):
        block_state(core, h)
    for h in range(heads):
        swaps[h].wait_recv()
        chip_sum[at_head(h), :] = states[core, at_head(h), :] + peer[at_head(h), :]

    def scan_rows(c):
        return pl.ds(pl.multiple_of(c * share, share), share)

    def scan_copy(src, dst, phase, to):
        return pltpu.make_async_remote_copy(
            src_ref=src,
            dst_ref=dst,
            send_sem=scan_sems.at[2 * phase],
            recv_sem=scan_sems.at[2 * phase + 1],
            device_id=(2 * to + core, head),
            device_id_type=MESH,
        )

    def await_scan(phase):
        all_of = gathered.at[pl.ds(0, chips - 1)]
        pltpu.make_async_copy(all_of, all_of, scan_sems.at[2 * phase + 1]).wait()

    for to in others:
        scan_copy(chip_sum.at[scan_rows(to)], gathered.at[chip], 0, to).start()
    gathered[chip] = chip_sum[scan_rows(chip), :]

    def scoring(h, _):
        score[h] = jnp.where(causal, product(unit[0, h], unit[1, h], NT), 0.0)
        peer_split[h] = left_parts(peer_other[h], 1)
        return 0

    for push in pushes:
        push.wait_recv()
    lax.fori_loop(0, heads, scoring, 0)
    await_scan(0)

    running = jnp.zeros((share, depth), F32)
    for i in range(chips):
        c = i + core * (chips - 1 - 2 * i)
        prefixes[c] = running
        running = running + gathered[c]

    for to in others:
        scan_copy(prefixes.at[to], entering.at[scan_rows(chip)], 1, to).start()
    entering[scan_rows(chip), :] = prefixes[chip]

    def inside(h, _):
        first[0, h] = product(score[h], other[1, h], NN)
        second[0, h] = product(mix[h], unit[1, h], NN)
        first[1, h] = product(score[h], other[0, h], TN)
        second[1, h] = product(mix[h], unit[0, h], TN)
        return 0

    lax.fori_loop(0, heads, inside, 0)
    inner = [jnp.zeros((tokens, depth), F32) for _ in range(2)]
    for h in range(heads):
        for i in range(2):
            inner[i] += unit[i, h] * second[i, h]
    share_sums(1, *inner)
    send_shares(1)
    await_scan(1)

    hands = [to_partner(passed, received, 1, h) for h in range(heads)]
    for h in range(heads):
        passed[at_head(h), :] = entering[at_head(h), :] + states[core, at_head(h), :]
        hands[h].start()

    def apply_first(which, state):
        def body(h, _):
            held = state[pl.ds(pl.multiple_of(h * depth, depth), depth), :]
            first[which, h] += product(unit[which, h], held, NT)
            return 0

        lax.fori_loop(0, heads, body, 0)

    own_inner = jnp.zeros((tokens, depth), F32)
    peer_inner = jnp.zeros((tokens, depth), F32)
    for h in range(heads):
        pushed = dot(split[core, h], right_parts(entering[at_head(h), :], 0), NN)
        second[core, h] += pushed
        own_inner += unit[core, h] * pushed
        peer_inner += peer_unit[h] * dot(peer_split[h], right_parts(passed[at_head(h), :], 0), NN)
    for kind, of_one in enumerate((own_inner, peer_inner)):
        sums = lane_sums(of_one)
        for j in range(tokens // 128):
            part_send[kind, pl.ds(j, 1), :] = sums[0:1, 128 * j : 128 * (j + 1)]
    for to in heads_on:
        part_copy(0, (seq, to)).start()
        part_copy(1, (peer_seq, to)).start()
    part_copy(1, partner).start()
    part_recv[0, head] = part_send[0]

    for h in range(heads):
        hands[h].wait_recv()
        second[1 - core, h] += dot(
            split[1 - core, h], right_parts(received[at_head(h), :], 0), NN
        )
    apply_first(core, entering)
    apply_first(1 - core, received)
    for h in range(heads):
        att_ref[rows_of(h), :] = first[0, h] * weight[...]
        gv_ref[rows_of(h), :] = first[1, h]
    for i in range(2):
        for h in range(heads):
            push_ref[i, h] = second[i, h] * gains[i, pl.ds(h, 1), :] * scales[i]
            base_ref[i, h] = raw[i, rows_of(h), :] * (scales[i] * scales[i])
    inside_total = await_shares(1)
    others_here = part_recv.at[0, pl.ds(0, n_head - 1)]
    pltpu.make_async_copy(others_here, others_here, part_sems.at[1]).wait()
    pltpu.make_async_copy(part_recv.at[1], part_recv.at[1], part_sems.at[3]).wait()
    own_part = jnp.sum(part_recv[0], axis=0)
    peer_part = jnp.sum(part_recv[1], axis=0)
    pairs = tokens // 128
    for i in range(2):
        rows = slice(pairs * i, pairs * (i + 1))
        part = jnp.where(core == i, own_part, peer_part * line_scale[rows, :])
        mean_ref[rows, :] = (inside_total[rows, :] + part) / width

    for h in range(heads):
        swaps[h].wait_send()
        hands[h].wait_send()
    for push in pushes:
        push.wait_send()
    pltpu.make_async_copy(others_here, others_here, part_sems.at[0]).wait()
    pltpu.make_async_copy(part_recv.at[1], part_recv.at[1], part_sems.at[2]).wait()
    for slot in range(2):
        all_of = z_recv.at[slot, pl.ds(0, n_head - 1)]
        pltpu.make_async_copy(all_of, all_of, z_sems.at[2 * slot]).wait()
    for phase in range(2):
        all_of = gathered.at[pl.ds(0, chips - 1)]
        pltpu.make_async_copy(all_of, all_of, scan_sems.at[2 * phase]).wait()


def leave(
    heads, tokens, att_ref, gv_ref, push_ref, base_ref, mean_ref,
    att_out, gq_out, gk_out, gv_out, staged, sems,
):
    copies = [
        pltpu.make_async_copy(src, dst, sems.at[i])
        for i, (src, dst) in enumerate(
            ((att_ref, att_out), (gv_ref, gv_out), (staged.at[0], gq_out), (staged.at[1], gk_out))
        )
    ]
    copies[0].start()
    copies[1].start()
    mean = mean_ref[...]
    for i in range(2):
        along = down_rows(mean, i, tokens)
        for h in range(heads):
            rows = pl.ds(h, tokens, stride=heads)
            staged[i, rows, :] = push_ref[i, h] - base_ref[i, h] * along
        copies[2 + i].start()
    for copy in copies:
        copy.wait()


def kept(x):
    return pltpu.with_memory_space_constraint(x, pltpu.HBM)


def local(n_seq, n_head, query_raw, key_raw, value_raw, query_gain, key_gain, cotangent):
    tokens, heads, depth = query_raw.shape
    chips = n_seq // 2
    flat = (tokens * heads, depth)
    both = (2, heads, tokens, depth)
    states = (heads * depth, depth)
    per_owner = (chips, heads * depth // chips, depth)
    hbm = pl.BlockSpec(memory_space=pltpu.HBM)
    vmem = pl.BlockSpec(memory_space=pltpu.VMEM)
    outs = pl.pallas_call(
        functools.partial(kernel, n_seq, n_head, heads, tokens, depth),
        out_shape=[
            jax.ShapeDtypeStruct(shape, F32)
            for shape in (flat, flat, both, both, (2 * tokens // 128, 128))
        ],
        in_specs=[hbm] * 6,
        out_specs=[vmem] * 5,
        scratch_shapes=[
            pltpu.VMEM((4, *flat), F32),
            pltpu.VMEM((2, heads, depth), F32),
            pltpu.VMEM(both, F32),
            pltpu.VMEM(both, F32),
            pltpu.VMEM((2, heads, depth, 3 * tokens), BF16),
            pltpu.VMEM((2, heads, tokens, 3 * depth), BF16),
            pltpu.VMEM(both, F32),
            pltpu.VMEM(both, F32),
            pltpu.VMEM((heads, tokens, tokens), F32),
            pltpu.VMEM((heads, tokens, tokens), F32),
            pltpu.VMEM((tokens, depth), F32),
            pltpu.VMEM((2, tokens, depth), F32),
            pltpu.VMEM((2, 2 * tokens // 128, 128), F32),
            pltpu.VMEM((2, n_head, 2 * tokens // 128, 128), F32),
            pltpu.VMEM((2, tokens // 128, 128), F32),
            pltpu.VMEM((2, n_head, tokens // 128, 128), F32),
            pltpu.VMEM((2 * tokens // 128, 128), F32),
            pltpu.VMEM(both[1:], F32),
            pltpu.VMEM(both[1:], F32),
            pltpu.VMEM(both[1:], F32),
            pltpu.VMEM((heads, tokens, 3 * depth), BF16),
            pltpu.VMEM((2, *states), F32),
            pltpu.VMEM(states, F32),
            pltpu.VMEM(states, F32),
            pltpu.VMEM(per_owner, F32),
            pltpu.VMEM(per_owner, F32),
            pltpu.VMEM(states, F32),
            pltpu.VMEM(states, F32),
            pltpu.VMEM(states, F32),
            pltpu.SemaphoreType.DMA((6,)),
            pltpu.SemaphoreType.DMA((4,)),
            pltpu.SemaphoreType.DMA((4,)),
            pltpu.SemaphoreType.DMA((4,)),
            pltpu.SemaphoreType.DMA((2, 2, heads)),
            pltpu.SemaphoreType.DMA((4,)),
        ],
        compiler_params=pltpu.CompilerParams(
            collective_id=0, has_side_effects=True, vmem_limit_bytes=48 * 1024 * 1024
        ),
    )(
        *(kept(x.reshape(flat)) for x in (query_raw, key_raw, value_raw, cotangent)),
        kept(query_gain),
        kept(key_gain),
    )
    outs = pl.pallas_call(
        functools.partial(leave, heads, tokens),
        out_shape=[jax.ShapeDtypeStruct(flat, F32)] * 4,
        in_specs=[vmem] * 5,
        out_specs=[hbm] * 4,
        scratch_shapes=[pltpu.VMEM((2, *flat), F32), pltpu.SemaphoreType.DMA((4,))],
        compiler_params=pltpu.CompilerParams(vmem_limit_bytes=4 * 1024 * 1024),
    )(*outs)
    return tuple(x.reshape(tokens, heads, depth) for x in outs)


def solution(mesh):
    spec, gain = P("seq", "head", None), P("head", None)
    return jax.shard_map(
        functools.partial(local, mesh.shape["seq"], mesh.shape["head"]),
        mesh=mesh,
        in_specs=(spec, spec, spec, gain, gain, spec),
        out_specs=(spec,) * 4,
        check_vma=False,
    )
```

```python
import functools

import jax
import jax.numpy as jnp
from jax import lax
from jax.experimental import pallas as pl
from jax.experimental.pallas import tpu as pltpu
from jax.sharding import PartitionSpec as P

MESH = pl.DeviceIdType.MESH
EPSILON = 1e-06
CHIPS_X = 4
F32, BF16 = jnp.float32, jnp.bfloat16

NN = ((1,), (0,))
NT = ((1,), (1,))
TN = ((0,), (0,))


def halves(x):
    high = x.astype(BF16)
    return high, (x - high.astype(F32)).astype(BF16)


def left_parts(x, axis):
    high, low = halves(x)
    return jnp.concatenate([high, low, high], axis=axis)


def right_parts(x, axis):
    high, low = halves(x)
    return jnp.concatenate([high, high, low], axis=axis)


def dot(left, right, form):
    return lax.dot_general(left, right, (form, ((), ())), preferred_element_type=F32)


def product(left, right, form):
    return dot(left_parts(left, form[0][0]), right_parts(right, form[1][0]), form)


def lane_sums(x):
    high, low = halves(x)
    rest = (x - high.astype(F32) - low.astype(F32)).astype(BF16)
    parts = jnp.concatenate([high, low, rest], axis=1)
    ones = jnp.ones((8, parts.shape[1]), BF16)
    return dot(ones, parts, NT)


def down_rows(line, i, tokens):
    return jnp.concatenate(
        [
            jnp.broadcast_to(line[2 * i + j : 2 * i + j + 1, :], (128, 128)).T
            for j in range(tokens // 128)
        ],
        axis=0,
    )


def kernel(
    n_seq, n_head, heads, tokens, depth,
    q_hbm, k_hbm, v_hbm, c_hbm, q_gain_hbm, k_gain_hbm,
    att_ref, gv_ref, push_ref, base_ref, mean_ref,
    raw, gains, unit, other, turned, split, first, second, mix, score, weight, scales,
    z_send, z_recv, z_cross, part_send, part_recv, line_scale, bare, peer_bare, peer_other,
    peer_split, peer_turned, states, chip_sum, gathered, prefixes, entering, passed, received,
    load_sem, z_sems, part_sems, push_sems, core_sems, scan_sems,
):
    chips = n_seq // 2
    share = heads * depth // chips
    seq, head = lax.axis_index("seq"), lax.axis_index("head")
    chip, core = seq // 2, seq % 2
    width = float(heads * n_head * depth)

    loads = [
        pltpu.make_async_copy(src, raw.at[i], load_sem.at[i])
        for i, src in enumerate((q_hbm, k_hbm, v_hbm, c_hbm))
    ] + [
        pltpu.make_async_copy(src, gains.at[i], load_sem.at[4 + i])
        for i, src in enumerate((q_gain_hbm, k_gain_hbm))
    ]
    for load in loads:
        load.start()

    barrier = pltpu.get_barrier_semaphore()

    chips_x = min(CHIPS_X, chips)
    chips_y = chips // chips_x
    chip_y, chip_x = chip // chips_x, chip % chips_x
    steps = sorted(
        [(dy, dx) for dy in range(chips_y) for dx in range(chips_x) if dy or dx],
        key=lambda s: -(min(s[0], chips_y - s[0]) + min(s[1], chips_x - s[1])),
    )
    others = [
        lax.rem(chip_y + dy, chips_y) * chips_x + lax.rem(chip_x + dx, chips_x) for dy, dx in steps
    ]
    heads_on = [
        lax.rem(head + d, n_head)
        for d in sorted(range(1, n_head), key=lambda d: -min(d, n_head - d))
    ]
    peer_seq = 2 * chip + 1 - core
    partner = (peer_seq, head)
    greeted = [(seq, to) for to in heads_on] + [(2 * to + core, head) for to in others]
    greeted += [(peer_seq, to) for to in heads_on] + [partner]
    for device in greeted:
        pl.semaphore_signal(barrier, inc=1, device_id=device, device_id_type=MESH)

    def rows_of(h):
        return pl.ds(h, tokens, stride=heads)

    def share_sums(slot, of_query, of_key):
        send, recv = z_send.at[slot], z_recv.at[slot]
        for i, of_one in enumerate((of_query, of_key)):
            sums = lane_sums(of_one)
            for j in range(tokens // 128):
                send[pl.ds(2 * i + j, 1), :] = sums[0:1, 128 * j : 128 * (j + 1)]
        recv[head] = send[...]

    def share_copy(slot, to):
        return pltpu.make_async_remote_copy(
            src_ref=z_send.at[slot],
            dst_ref=z_recv.at[slot, head],
            send_sem=z_sems.at[2 * slot],
            recv_sem=z_sems.at[2 * slot + 1],
            device_id=(seq, to),
            device_id_type=MESH,
        )

    def send_shares(slot):
        for to in heads_on:
            share_copy(slot, to).start()

    def cross_copy(to):
        return pltpu.make_async_remote_copy(
            src_ref=z_send.at[0],
            dst_ref=z_cross.at[head],
            send_sem=z_sems.at[4],
            recv_sem=z_sems.at[5],
            device_id=(peer_seq, to),
            device_id_type=MESH,
        )

    def part_copy(kind, device):
        return pltpu.make_async_remote_copy(
            src_ref=part_send.at[kind],
            dst_ref=part_recv.at[kind, head],
            send_sem=part_sems.at[2 * kind],
            recv_sem=part_sems.at[2 * kind + 1],
            device_id=device,
            device_id_type=MESH,
        )

    def await_shares(slot):
        all_of = z_recv.at[slot, pl.ds(0, n_head - 1)]
        pltpu.make_async_copy(all_of, all_of, z_sems.at[2 * slot + 1]).wait()
        return jnp.sum(z_recv[slot], axis=0)

    loads[0].wait()
    loads[1].wait()
    query_squares = jnp.zeros((tokens, depth), F32)
    key_squares = jnp.zeros((tokens, depth), F32)
    for h in range(heads):
        q, k = raw[0, rows_of(h), :], raw[1, rows_of(h), :]
        query_squares += q * q
        key_squares += k * k
    share_sums(0, query_squares, key_squares)

    pl.semaphore_wait(barrier, len(greeted))
    for to in heads_on:
        share_copy(0, to).start()
        cross_copy(to).start()
    cross_copy(head).start()

    loads[2].wait()
    loads[3].wait()
    loads[4].wait()
    loads[5].wait()
    position = (seq * tokens + lax.broadcasted_iota(jnp.int32, (tokens, depth), 0)).astype(F32)
    weight[...] = lax.rsqrt(float(depth) * (position + 1.0))
    for h in range(heads):
        other[0, h] = raw[3, rows_of(h), :] * weight[...]
        other[1, h] = raw[2, rows_of(h), :]
    for i in range(2):
        for h in range(heads):
            bare[i, h] = raw[i, rows_of(h), :] * gains[i, pl.ds(h, 1), :]

    pushes = [
        pltpu.make_async_remote_copy(
            src_ref=src,
            dst_ref=dst,
            send_sem=push_sems.at[2 * i],
            recv_sem=push_sems.at[2 * i + 1],
            device_id=partner,
            device_id_type=MESH,
        )
        for i, (src, dst) in enumerate(
            ((other, peer_other), (bare, peer_bare))
        )
    ]
    for push in pushes:
        push.start()

    def turning(h, _):
        for i in range(2):
            turned[i, h] = left_parts(other[i, h].T, 1)
            split[i, h] = left_parts(other[i, h], 1)
        return 0

    lax.fori_loop(0, heads, turning, 0)

    rows = lax.broadcasted_iota(jnp.int32, (tokens, tokens), 0)
    columns = lax.broadcasted_iota(jnp.int32, (tokens, tokens), 1)
    causal = rows >= columns

    def mixing(h, _):
        mix[h] = jnp.where(causal, product(other[0, h], other[1, h], NT), 0.0)
        return 0

    lax.fori_loop(0, heads, mixing, 0)

    for push in pushes:
        push.wait_recv()

    def turning_peer(h, _):
        peer_turned[h] = left_parts(peer_other[1 - core, h].T, 1)
        return 0

    lax.fori_loop(0, heads, turning_peer, 0)

    def scale_of(total):
        return lax.rsqrt(total / width + EPSILON)

    def at_head(h):
        return pl.ds(h * depth, depth)

    pairs = tokens // 128

    def of_kind(lines, first_kind):
        return jnp.where(first_kind, lines[:pairs, :], lines[pairs:, :])

    scale = scale_of(await_shares(0))
    pltpu.make_async_copy(z_cross, z_cross, z_sems.at[5]).wait()
    peer_scale = scale_of(jnp.sum(z_cross[...], axis=0))
    line_scale[...] = scale
    down = down_rows(of_kind(scale, core == 1), 0, tokens)
    peer_down = down_rows(of_kind(peer_scale, core == 1), 0, tokens)
    scales[1 - core] = down
    for h in range(heads):
        normed = right_parts(bare[1 - core, h] * down, 0)
        peer_normed = right_parts(peer_bare[1 - core, h] * peer_down, 0)
        chip_sum[at_head(h), :] = dot(
            jnp.concatenate([turned[1 - core, h], peer_turned[h]], axis=1),
            jnp.concatenate([normed, peer_normed], axis=0),
            NN,
        )

    def to_partner(src, dst, h):
        return pltpu.make_async_remote_copy(
            src_ref=src.at[at_head(h)],
            dst_ref=dst.at[at_head(h)],
            send_sem=core_sems.at[0, h],
            recv_sem=core_sems.at[1, h],
            device_id=partner,
            device_id_type=MESH,
        )

    def scan_rows(c):
        return pl.ds(pl.multiple_of(c * share, share), share)

    def scan_copy(src, dst, phase, to):
        return pltpu.make_async_remote_copy(
            src_ref=src,
            dst_ref=dst,
            send_sem=scan_sems.at[2 * phase],
            recv_sem=scan_sems.at[2 * phase + 1],
            device_id=(2 * to + core, head),
            device_id_type=MESH,
        )

    def await_scan(phase):
        all_of = gathered.at[pl.ds(0, chips - 1)]
        pltpu.make_async_copy(all_of, all_of, scan_sems.at[2 * phase + 1]).wait()

    for to in others:
        scan_copy(chip_sum.at[scan_rows(to)], gathered.at[chip], 0, to).start()
    gathered[chip] = chip_sum[scan_rows(chip), :]

    def scoring(h, _):
        for i in range(2):
            unit[i, h] = bare[i, h] * scales[i]
        states[pl.ds(pl.multiple_of(h * depth, depth), depth), :] = dot(
            turned[1 - core, h], right_parts(unit[1 - core, h], 0), NN
        )
        score[h] = jnp.where(causal, product(unit[0, h], unit[1, h], NT), 0.0)
        peer_split[h] = left_parts(peer_other[core, h], 1)
        return 0

    scales[core] = down_rows(of_kind(scale, core == 0), 0, tokens)
    lax.fori_loop(0, heads, scoring, 0)
    await_scan(0)

    running = jnp.zeros((share, depth), F32)
    for i in range(chips):
        c = i + core * (chips - 1 - 2 * i)
        prefixes[c] = running
        running = running + gathered[c]

    for to in others:
        scan_copy(prefixes.at[to], entering.at[scan_rows(chip)], 1, to).start()
    entering[scan_rows(chip), :] = prefixes[chip]

    def inside(h, _):
        first[0, h] = product(score[h], other[1, h], NN)
        second[0, h] = product(mix[h], unit[1, h], NN)
        first[1, h] = product(score[h], other[0, h], TN)
        second[1, h] = product(mix[h], unit[0, h], TN)
        return 0

    lax.fori_loop(0, heads, inside, 0)
    inner = [jnp.zeros((tokens, depth), F32) for _ in range(2)]
    for h in range(heads):
        for i in range(2):
            inner[i] += unit[i, h] * second[i, h]
    share_sums(1, *inner)
    send_shares(1)
    await_scan(1)

    hands = [to_partner(passed, received, h) for h in range(heads)]
    for h in range(heads):
        passed[at_head(h), :] = entering[at_head(h), :] + states[at_head(h), :]
        hands[h].start()

    def apply_first(which, state):
        def body(h, _):
            held = state[pl.ds(pl.multiple_of(h * depth, depth), depth), :]
            first[which, h] += product(unit[which, h], held, NT)
            return 0

        lax.fori_loop(0, heads, body, 0)

    own_inner = jnp.zeros((tokens, depth), F32)
    peer_inner = jnp.zeros((tokens, depth), F32)
    for h in range(heads):
        pushed = dot(split[core, h], right_parts(entering[at_head(h), :], 0), NN)
        second[core, h] += pushed
        own_inner += unit[core, h] * pushed
        peer_inner += peer_bare[core, h] * dot(peer_split[h], right_parts(passed[at_head(h), :], 0), NN)
    for kind, of_one in enumerate((own_inner, peer_inner)):
        sums = lane_sums(of_one)
        for j in range(tokens // 128):
            part_send[kind, pl.ds(j, 1), :] = sums[0:1, 128 * j : 128 * (j + 1)]
    for to in heads_on:
        part_copy(0, (seq, to)).start()
        part_copy(1, (peer_seq, to)).start()
    part_copy(1, partner).start()
    part_recv[0, head] = part_send[0]

    for h in range(heads):
        hands[h].wait_recv()
        second[1 - core, h] += dot(
            split[1 - core, h], right_parts(received[at_head(h), :], 0), NN
        )
    apply_first(core, entering)
    apply_first(1 - core, received)
    for h in range(heads):
        att_ref[rows_of(h), :] = first[0, h] * weight[...]
        gv_ref[rows_of(h), :] = first[1, h]
    for i in range(2):
        for h in range(heads):
            push_ref[i, h] = second[i, h] * gains[i, pl.ds(h, 1), :] * scales[i]
            base_ref[i, h] = raw[i, rows_of(h), :] * (scales[i] * scales[i])
    inside_total = await_shares(1)
    others_here = part_recv.at[0, pl.ds(0, n_head - 1)]
    pltpu.make_async_copy(others_here, others_here, part_sems.at[1]).wait()
    pltpu.make_async_copy(part_recv.at[1], part_recv.at[1], part_sems.at[3]).wait()
    own_part = jnp.sum(part_recv[0], axis=0)
    peer_part = jnp.sum(part_recv[1], axis=0)
    for i in range(2):
        rows = slice(pairs * i, pairs * (i + 1))
        part = jnp.where(core == i, own_part, peer_part * line_scale[rows, :])
        mean_ref[rows, :] = (inside_total[rows, :] + part) / width

    for h in range(heads):
        hands[h].wait_send()
    for push in pushes:
        push.wait_send()
    pltpu.make_async_copy(others_here, others_here, part_sems.at[0]).wait()
    pltpu.make_async_copy(part_recv.at[1], part_recv.at[1], part_sems.at[2]).wait()
    pltpu.make_async_copy(z_cross, z_cross, z_sems.at[4]).wait()
    for slot in range(2):
        all_of = z_recv.at[slot, pl.ds(0, n_head - 1)]
        pltpu.make_async_copy(all_of, all_of, z_sems.at[2 * slot]).wait()
    for phase in range(2):
        all_of = gathered.at[pl.ds(0, chips - 1)]
        pltpu.make_async_copy(all_of, all_of, scan_sems.at[2 * phase]).wait()


def leave(
    heads, tokens, att_ref, gv_ref, push_ref, base_ref, mean_ref,
    att_out, gq_out, gk_out, gv_out, staged, sems,
):
    copies = [
        pltpu.make_async_copy(src, dst, sems.at[i])
        for i, (src, dst) in enumerate(
            ((att_ref, att_out), (gv_ref, gv_out), (staged.at[0], gq_out), (staged.at[1], gk_out))
        )
    ]
    copies[0].start()
    copies[1].start()
    mean = mean_ref[...]
    for i in range(2):
        along = down_rows(mean, i, tokens)
        for h in range(heads):
            rows = pl.ds(h, tokens, stride=heads)
            staged[i, rows, :] = push_ref[i, h] - base_ref[i, h] * along
        copies[2 + i].start()
    for copy in copies:
        copy.wait()


def kept(x):
    return pltpu.with_memory_space_constraint(x, pltpu.HBM)


def local(n_seq, n_head, query_raw, key_raw, value_raw, query_gain, key_gain, cotangent):
    tokens, heads, depth = query_raw.shape
    chips = n_seq // 2
    flat = (tokens * heads, depth)
    both = (2, heads, tokens, depth)
    states = (heads * depth, depth)
    per_owner = (chips, heads * depth // chips, depth)
    hbm = pl.BlockSpec(memory_space=pltpu.HBM)
    vmem = pl.BlockSpec(memory_space=pltpu.VMEM)
    outs = pl.pallas_call(
        functools.partial(kernel, n_seq, n_head, heads, tokens, depth),
        out_shape=[
            jax.ShapeDtypeStruct(shape, F32)
            for shape in (flat, flat, both, both, (2 * tokens // 128, 128))
        ],
        in_specs=[hbm] * 6,
        out_specs=[vmem] * 5,
        scratch_shapes=[
            pltpu.VMEM((4, *flat), F32),
            pltpu.VMEM((2, heads, depth), F32),
            pltpu.VMEM(both, F32),
            pltpu.VMEM(both, F32),
            pltpu.VMEM((2, heads, depth, 3 * tokens), BF16),
            pltpu.VMEM((2, heads, tokens, 3 * depth), BF16),
            pltpu.VMEM(both, F32),
            pltpu.VMEM(both, F32),
            pltpu.VMEM((heads, tokens, tokens), F32),
            pltpu.VMEM((heads, tokens, tokens), F32),
            pltpu.VMEM((tokens, depth), F32),
            pltpu.VMEM((2, tokens, depth), F32),
            pltpu.VMEM((2, 2 * tokens // 128, 128), F32),
            pltpu.VMEM((2, n_head, 2 * tokens // 128, 128), F32),
            pltpu.VMEM((n_head, 2 * tokens // 128, 128), F32),
            pltpu.VMEM((2, tokens // 128, 128), F32),
            pltpu.VMEM((2, n_head, tokens // 128, 128), F32),
            pltpu.VMEM((2 * tokens // 128, 128), F32),
            pltpu.VMEM(both, F32),
            pltpu.VMEM(both, F32),
            pltpu.VMEM(both, F32),
            pltpu.VMEM((heads, tokens, 3 * depth), BF16),
            pltpu.VMEM((heads, depth, 3 * tokens), BF16),
            pltpu.VMEM(states, F32),
            pltpu.VMEM(states, F32),
            pltpu.VMEM(per_owner, F32),
            pltpu.VMEM(per_owner, F32),
            pltpu.VMEM(states, F32),
            pltpu.VMEM(states, F32),
            pltpu.VMEM(states, F32),
            pltpu.SemaphoreType.DMA((6,)),
            pltpu.SemaphoreType.DMA((6,)),
            pltpu.SemaphoreType.DMA((4,)),
            pltpu.SemaphoreType.DMA((4,)),
            pltpu.SemaphoreType.DMA((2, heads)),
            pltpu.SemaphoreType.DMA((4,)),
        ],
        compiler_params=pltpu.CompilerParams(
            collective_id=0, has_side_effects=True, vmem_limit_bytes=48 * 1024 * 1024
        ),
    )(
        *(kept(x.reshape(flat)) for x in (query_raw, key_raw, value_raw, cotangent)),
        kept(query_gain),
        kept(key_gain),
    )
    outs = pl.pallas_call(
        functools.partial(leave, heads, tokens),
        out_shape=[jax.ShapeDtypeStruct(flat, F32)] * 4,
        in_specs=[vmem] * 5,
        out_specs=[hbm] * 4,
        scratch_shapes=[pltpu.VMEM((2, *flat), F32), pltpu.SemaphoreType.DMA((4,))],
        compiler_params=pltpu.CompilerParams(vmem_limit_bytes=4 * 1024 * 1024),
    )(*outs)
    return tuple(x.reshape(tokens, heads, depth) for x in outs)


def solution(mesh):
    spec, gain = P("seq", "head", None), P("head", None)
    return jax.shard_map(
        functools.partial(local, mesh.shape["seq"], mesh.shape["head"]),
        mesh=mesh,
        in_specs=(spec, spec, spec, gain, gain, spec),
        out_specs=(spec,) * 4,
        check_vma=False,
    )
```

```python
import functools

import jax
import jax.numpy as jnp
from jax import lax
from jax.experimental import pallas as pl
from jax.experimental.pallas import tpu as pltpu
from jax.sharding import PartitionSpec as P

MESH = pl.DeviceIdType.MESH
EPSILON = 1e-06
CHIPS_X = 4
F32, BF16 = jnp.float32, jnp.bfloat16

NN = ((1,), (0,))
NT = ((1,), (1,))
TN = ((0,), (0,))


def halves(x):
    high = x.astype(BF16)
    return high, (x - high.astype(F32)).astype(BF16)


def left_parts(x, axis):
    high, low = halves(x)
    return jnp.concatenate([high, low, high], axis=axis)


def right_parts(x, axis):
    high, low = halves(x)
    return jnp.concatenate([high, high, low], axis=axis)


def dot(left, right, form):
    return lax.dot_general(left, right, (form, ((), ())), preferred_element_type=F32)


def product(left, right, form):
    return dot(left_parts(left, form[0][0]), right_parts(right, form[1][0]), form)


def lane_sums(x):
    high, low = halves(x)
    rest = (x - high.astype(F32) - low.astype(F32)).astype(BF16)
    parts = jnp.concatenate([high, low, rest], axis=1)
    ones = jnp.ones((8, parts.shape[1]), BF16)
    return dot(ones, parts, NT)


def down_rows(line, i, tokens):
    return jnp.concatenate(
        [
            jnp.broadcast_to(line[2 * i + j : 2 * i + j + 1, :], (128, 128)).T
            for j in range(tokens // 128)
        ],
        axis=0,
    )


def kernel(
    n_seq, n_head, heads, tokens, depth,
    q_hbm, k_hbm, v_hbm, c_hbm, q_gain_hbm, k_gain_hbm,
    att_ref, gv_ref, push_ref, base_ref, mean_ref,
    raw, gains, unit, other, turned, split, first, second, mix, score, weight, scales,
    z_send, z_recv, z_cross, part_send, part_recv, line_scale, bare, peer_bare, peer_other,
    peer_split, peer_turned, states, chip_sum, gathered, prefixes, entering, passed, received,
    load_sem, z_sems, part_sems, push_sems, core_sems, scan_sems, give_sems,
):
    chips = n_seq // 2
    share = heads * depth // chips
    seq, head = lax.axis_index("seq"), lax.axis_index("head")
    chip, core = seq // 2, seq % 2
    width = float(heads * n_head * depth)

    loads = [
        pltpu.make_async_copy(src, raw.at[i], load_sem.at[i])
        for i, src in enumerate((q_hbm, k_hbm, v_hbm, c_hbm))
    ] + [
        pltpu.make_async_copy(src, gains.at[i], load_sem.at[4 + i])
        for i, src in enumerate((q_gain_hbm, k_gain_hbm))
    ]
    barrier = pltpu.get_barrier_semaphore()

    chips_x = min(CHIPS_X, chips)
    chips_y = chips // chips_x
    chip_y, chip_x = chip // chips_x, chip % chips_x
    steps = sorted(
        [(dy, dx) for dy in range(chips_y) for dx in range(chips_x) if dy or dx],
        key=lambda s: -(min(s[0], chips_y - s[0]) + min(s[1], chips_x - s[1])),
    )
    others = [
        lax.rem(chip_y + dy, chips_y) * chips_x + lax.rem(chip_x + dx, chips_x) for dy, dx in steps
    ]
    turns = sorted(range(1, n_head), key=lambda d: -min(d, n_head - d))
    heads_on = [lax.rem(head + d, n_head) for d in turns]
    peer_seq = 2 * chip + 1 - core
    partner = (peer_seq, head)
    greeted = [(0, partner)]
    for d, to in zip(turns, heads_on):
        greeted += [(min(d, n_head - d), (at, to)) for at in (seq, peer_seq)]
    for (dy, dx), to in zip(steps, others):
        hops = min(dy, chips_y - dy) + min(dx, chips_x - dx)
        greeted.append((hops, (2 * to + core, head)))
    for _, device in sorted(greeted, key=lambda pair: -pair[0]):
        pl.semaphore_signal(barrier, inc=1, device_id=device, device_id_type=MESH)
    for load in loads:
        load.start()

    def rows_of(h):
        return pl.ds(h, tokens, stride=heads)

    def share_sums(slot, of_query, of_key):
        send, recv = z_send.at[slot], z_recv.at[slot]
        for i, of_one in enumerate((of_query, of_key)):
            sums = lane_sums(of_one)
            for j in range(tokens // 128):
                send[pl.ds(2 * i + j, 1), :] = sums[0:1, 128 * j : 128 * (j + 1)]
        recv[head] = send[...]

    def share_copy(slot, to):
        return pltpu.make_async_remote_copy(
            src_ref=z_send.at[slot],
            dst_ref=z_recv.at[slot, head],
            send_sem=z_sems.at[2 * slot],
            recv_sem=z_sems.at[2 * slot + 1],
            device_id=(seq, to),
            device_id_type=MESH,
        )

    def send_shares(slot):
        for to in heads_on:
            share_copy(slot, to).start()

    def cross_copy(to):
        return pltpu.make_async_remote_copy(
            src_ref=z_send.at[0],
            dst_ref=z_cross.at[head],
            send_sem=z_sems.at[4],
            recv_sem=z_sems.at[5],
            device_id=(peer_seq, to),
            device_id_type=MESH,
        )

    def part_copy(kind, device):
        return pltpu.make_async_remote_copy(
            src_ref=part_send.at[kind],
            dst_ref=part_recv.at[kind, head],
            send_sem=part_sems.at[2 * kind],
            recv_sem=part_sems.at[2 * kind + 1],
            device_id=device,
            device_id_type=MESH,
        )

    def await_shares(slot):
        all_of = z_recv.at[slot, pl.ds(0, n_head - 1)]
        pltpu.make_async_copy(all_of, all_of, z_sems.at[2 * slot + 1]).wait()
        return jnp.sum(z_recv[slot], axis=0)

    loads[0].wait()
    loads[1].wait()
    query_squares = jnp.zeros((tokens, depth), F32)
    key_squares = jnp.zeros((tokens, depth), F32)
    for h in range(heads):
        q, k = raw[0, rows_of(h), :], raw[1, rows_of(h), :]
        query_squares += q * q
        key_squares += k * k
    share_sums(0, query_squares, key_squares)

    pl.semaphore_wait(barrier, len(greeted))
    for to in heads_on:
        share_copy(0, to).start()
        cross_copy(to).start()
    cross_copy(head).start()

    loads[2].wait()
    loads[3].wait()
    loads[4].wait()
    loads[5].wait()
    position = (seq * tokens + lax.broadcasted_iota(jnp.int32, (tokens, depth), 0)).astype(F32)
    weight[...] = lax.rsqrt(float(depth) * (position + 1.0))
    for h in range(heads):
        other[0, h] = raw[3, rows_of(h), :] * weight[...]
        other[1, h] = raw[2, rows_of(h), :]
    for i in range(2):
        for h in range(heads):
            bare[i, h] = raw[i, rows_of(h), :] * gains[i, pl.ds(h, 1), :]

    pushes = [
        pltpu.make_async_remote_copy(
            src_ref=src,
            dst_ref=dst,
            send_sem=push_sems.at[2 * i],
            recv_sem=push_sems.at[2 * i + 1],
            device_id=partner,
            device_id_type=MESH,
        )
        for i, (src, dst) in enumerate(
            ((other, peer_other), (bare, peer_bare))
        )
    ]
    for push in pushes:
        push.start()

    def turning(h, _):
        for i in range(2):
            turned[i, h] = left_parts(other[i, h].T, 1)
            split[i, h] = left_parts(other[i, h], 1)
        return 0

    lax.fori_loop(0, heads, turning, 0)

    rows = lax.broadcasted_iota(jnp.int32, (tokens, tokens), 0)
    columns = lax.broadcasted_iota(jnp.int32, (tokens, tokens), 1)
    causal = rows >= columns

    def mixing(h, _):
        mix[h] = jnp.where(causal, product(other[0, h], other[1, h], NT), 0.0)
        return 0

    lax.fori_loop(0, heads, mixing, 0)

    for push in pushes:
        push.wait_recv()

    def turning_peer(h, _):
        peer_turned[h] = left_parts(peer_other[1 - core, h].T, 1)
        return 0

    lax.fori_loop(0, heads, turning_peer, 0)

    def scale_of(total):
        return lax.rsqrt(total / width + EPSILON)

    def at_head(h):
        return pl.ds(h * depth, depth)

    pairs = tokens // 128

    def of_kind(lines, first_kind):
        return jnp.where(first_kind, lines[:pairs, :], lines[pairs:, :])

    scale = scale_of(await_shares(0))
    pltpu.make_async_copy(z_cross, z_cross, z_sems.at[5]).wait()
    peer_scale = scale_of(jnp.sum(z_cross[...], axis=0))
    line_scale[...] = scale
    down = down_rows(of_kind(scale, core == 1), 0, tokens)
    peer_down = down_rows(of_kind(peer_scale, core == 1), 0, tokens)
    scales[1 - core] = down
    for h in range(heads):
        normed = right_parts(bare[1 - core, h] * down, 0)
        peer_normed = right_parts(peer_bare[1 - core, h] * peer_down, 0)
        chip_sum[at_head(h), :] = dot(
            jnp.concatenate([turned[1 - core, h], peer_turned[h]], axis=1),
            jnp.concatenate([normed, peer_normed], axis=0),
            NN,
        )

    def to_partner(src, dst, h):
        return pltpu.make_async_remote_copy(
            src_ref=src.at[at_head(h)],
            dst_ref=dst.at[at_head(h)],
            send_sem=core_sems.at[0, h],
            recv_sem=core_sems.at[1, h],
            device_id=partner,
            device_id_type=MESH,
        )

    def scan_rows(c):
        return pl.ds(pl.multiple_of(c * share, share), share)

    def scan_copy(src, dst, send_sem, recv_sem, to):
        return pltpu.make_async_remote_copy(
            src_ref=src,
            dst_ref=dst,
            send_sem=send_sem,
            recv_sem=recv_sem,
            device_id=(2 * to + core, head),
            device_id_type=MESH,
        )

    per_head = chips // heads
    block = chip // per_head

    for to in others:
        scan_copy(
            chip_sum.at[scan_rows(to)], gathered.at[chip], scan_sems.at[0], scan_sems.at[1], to
        ).start()
    gathered[chip] = chip_sum[scan_rows(chip), :]

    def scoring(h, _):
        for i in range(2):
            unit[i, h] = bare[i, h] * scales[i]
        states[pl.ds(pl.multiple_of(h * depth, depth), depth), :] = dot(
            turned[1 - core, h], right_parts(unit[1 - core, h], 0), NN
        )
        score[h] = jnp.where(causal, product(unit[0, h], unit[1, h], NT), 0.0)
        peer_split[h] = left_parts(peer_other[core, h], 1)
        return 0

    scales[core] = down_rows(of_kind(scale, core == 0), 0, tokens)
    lax.fori_loop(0, heads, scoring, 0)
    all_others = gathered.at[pl.ds(0, chips - 1)]
    pltpu.make_async_copy(all_others, all_others, scan_sems.at[1]).wait()

    running = jnp.zeros((share, depth), F32)
    for i in range(chips):
        c = i + core * (chips - 1 - 2 * i)
        prefixes[c] = running
        running = running + gathered[c]

    for to in others:
        scan_copy(
            prefixes.at[to],
            entering.at[scan_rows(chip)],
            give_sems.at[heads],
            give_sems.at[block],
            to,
        ).start()
    pltpu.make_async_copy(
        prefixes.at[chip], entering.at[scan_rows(chip)], give_sems.at[block]
    ).start()

    def inside(h, _):
        first[0, h] = product(score[h], other[1, h], NN)
        second[0, h] = product(mix[h], unit[1, h], NN)
        first[1, h] = product(score[h], other[0, h], TN)
        second[1, h] = product(mix[h], unit[0, h], TN)
        return 0

    lax.fori_loop(0, heads, inside, 0)
    inner = [jnp.zeros((tokens, depth), F32) for _ in range(2)]
    for h in range(heads):
        for i in range(2):
            inner[i] += unit[i, h] * second[i, h]
    share_sums(1, *inner)
    send_shares(1)
    def apply_first(which, state):
        def body(h, _):
            held = state[pl.ds(pl.multiple_of(h * depth, depth), depth), :]
            first[which, h] += product(unit[which, h], held, NT)
            return 0

        lax.fori_loop(0, heads, body, 0)

    own_inner = jnp.zeros((tokens, depth), F32)
    peer_inner = jnp.zeros((tokens, depth), F32)
    for far in sorted(range(heads), key=lambda k: -min(k, heads - k)):
        h = lax.rem(block + far, heads)
        here = pl.ds(pl.multiple_of(h * depth, depth), depth)
        one_head = gathered.at[pl.ds(0, per_head)]
        pltpu.make_async_copy(one_head, one_head, give_sems.at[h]).wait()
        held = entering[here, :]
        next_held = held + states[here, :]
        passed[here, :] = next_held
        pushed = dot(split[core, h], right_parts(held, 0), NN)
        second[core, h] += pushed
        own_inner += unit[core, h] * pushed
        peer_inner += peer_bare[core, h] * dot(peer_split[h], right_parts(next_held, 0), NN)
    hands = [to_partner(passed, received, h) for h in range(heads)]
    for kind, of_one in enumerate((own_inner, peer_inner)):
        sums = lane_sums(of_one)
        for j in range(tokens // 128):
            part_send[kind, pl.ds(j, 1), :] = sums[0:1, 128 * j : 128 * (j + 1)]
    for to in heads_on:
        part_copy(0, (seq, to)).start()
        part_copy(1, (peer_seq, to)).start()
    part_copy(1, partner).start()
    part_recv[0, head] = part_send[0]
    for hand in hands:
        hand.start()

    for h in range(heads):
        hands[h].wait_recv()
        second[1 - core, h] += dot(
            split[1 - core, h], right_parts(received[at_head(h), :], 0), NN
        )
    apply_first(core, entering)
    apply_first(1 - core, received)
    for h in range(heads):
        att_ref[rows_of(h), :] = first[0, h] * weight[...]
        gv_ref[rows_of(h), :] = first[1, h]
    for i in range(2):
        for h in range(heads):
            push_ref[i, h] = second[i, h] * gains[i, pl.ds(h, 1), :] * scales[i]
            base_ref[i, h] = raw[i, rows_of(h), :] * (scales[i] * scales[i])
    inside_total = await_shares(1)
    others_here = part_recv.at[0, pl.ds(0, n_head - 1)]
    pltpu.make_async_copy(others_here, others_here, part_sems.at[1]).wait()
    pltpu.make_async_copy(part_recv.at[1], part_recv.at[1], part_sems.at[3]).wait()
    own_part = jnp.sum(part_recv[0], axis=0)
    peer_part = jnp.sum(part_recv[1], axis=0)
    for i in range(2):
        rows = slice(pairs * i, pairs * (i + 1))
        part = jnp.where(core == i, own_part, peer_part * line_scale[rows, :])
        mean_ref[rows, :] = (inside_total[rows, :] + part) / width

    for h in range(heads):
        hands[h].wait_send()
    for push in pushes:
        push.wait_send()
    pltpu.make_async_copy(others_here, others_here, part_sems.at[0]).wait()
    pltpu.make_async_copy(part_recv.at[1], part_recv.at[1], part_sems.at[2]).wait()
    pltpu.make_async_copy(z_cross, z_cross, z_sems.at[4]).wait()
    for slot in range(2):
        all_of = z_recv.at[slot, pl.ds(0, n_head - 1)]
        pltpu.make_async_copy(all_of, all_of, z_sems.at[2 * slot]).wait()
    for sem in (scan_sems.at[0], give_sems.at[heads]):
        pltpu.make_async_copy(all_others, all_others, sem).wait()


def leave(
    heads, tokens, att_ref, gv_ref, push_ref, base_ref, mean_ref,
    att_out, gq_out, gk_out, gv_out, staged, sems,
):
    copies = [
        pltpu.make_async_copy(src, dst, sems.at[i])
        for i, (src, dst) in enumerate(
            ((att_ref, att_out), (gv_ref, gv_out), (staged.at[0], gq_out), (staged.at[1], gk_out))
        )
    ]
    copies[0].start()
    copies[1].start()
    mean = mean_ref[...]
    for i in range(2):
        along = down_rows(mean, i, tokens)
        for h in range(heads):
            rows = pl.ds(h, tokens, stride=heads)
            staged[i, rows, :] = push_ref[i, h] - base_ref[i, h] * along
        copies[2 + i].start()
    for copy in copies:
        copy.wait()


def kept(x):
    return pltpu.with_memory_space_constraint(x, pltpu.HBM)


def local(n_seq, n_head, query_raw, key_raw, value_raw, query_gain, key_gain, cotangent):
    tokens, heads, depth = query_raw.shape
    chips = n_seq // 2
    flat = (tokens * heads, depth)
    both = (2, heads, tokens, depth)
    states = (heads * depth, depth)
    per_owner = (chips, heads * depth // chips, depth)
    hbm = pl.BlockSpec(memory_space=pltpu.HBM)
    vmem = pl.BlockSpec(memory_space=pltpu.VMEM)
    outs = pl.pallas_call(
        functools.partial(kernel, n_seq, n_head, heads, tokens, depth),
        out_shape=[
            jax.ShapeDtypeStruct(shape, F32)
            for shape in (flat, flat, both, both, (2 * tokens // 128, 128))
        ],
        in_specs=[hbm] * 6,
        out_specs=[vmem] * 5,
        scratch_shapes=[
            pltpu.VMEM((4, *flat), F32),
            pltpu.VMEM((2, heads, depth), F32),
            pltpu.VMEM(both, F32),
            pltpu.VMEM(both, F32),
            pltpu.VMEM((2, heads, depth, 3 * tokens), BF16),
            pltpu.VMEM((2, heads, tokens, 3 * depth), BF16),
            pltpu.VMEM(both, F32),
            pltpu.VMEM(both, F32),
            pltpu.VMEM((heads, tokens, tokens), F32),
            pltpu.VMEM((heads, tokens, tokens), F32),
            pltpu.VMEM((tokens, depth), F32),
            pltpu.VMEM((2, tokens, depth), F32),
            pltpu.VMEM((2, 2 * tokens // 128, 128), F32),
            pltpu.VMEM((2, n_head, 2 * tokens // 128, 128), F32),
            pltpu.VMEM((n_head, 2 * tokens // 128, 128), F32),
            pltpu.VMEM((2, tokens // 128, 128), F32),
            pltpu.VMEM((2, n_head, tokens // 128, 128), F32),
            pltpu.VMEM((2 * tokens // 128, 128), F32),
            pltpu.VMEM(both, F32),
            pltpu.VMEM(both, F32),
            pltpu.VMEM(both, F32),
            pltpu.VMEM((heads, tokens, 3 * depth), BF16),
            pltpu.VMEM((heads, depth, 3 * tokens), BF16),
            pltpu.VMEM(states, F32),
            pltpu.VMEM(states, F32),
            pltpu.VMEM(per_owner, F32),
            pltpu.VMEM(per_owner, F32),
            pltpu.VMEM(states, F32),
            pltpu.VMEM(states, F32),
            pltpu.VMEM(states, F32),
            pltpu.SemaphoreType.DMA((6,)),
            pltpu.SemaphoreType.DMA((6,)),
            pltpu.SemaphoreType.DMA((4,)),
            pltpu.SemaphoreType.DMA((4,)),
            pltpu.SemaphoreType.DMA((2, heads)),
            pltpu.SemaphoreType.DMA((2,)),
            pltpu.SemaphoreType.DMA((heads + 1,)),
        ],
        compiler_params=pltpu.CompilerParams(
            collective_id=0, has_side_effects=True, vmem_limit_bytes=48 * 1024 * 1024
        ),
    )(
        *(kept(x.reshape(flat)) for x in (query_raw, key_raw, value_raw, cotangent)),
        kept(query_gain),
        kept(key_gain),
    )
    outs = pl.pallas_call(
        functools.partial(leave, heads, tokens),
        out_shape=[jax.ShapeDtypeStruct(flat, F32)] * 4,
        in_specs=[vmem] * 5,
        out_specs=[hbm] * 4,
        scratch_shapes=[pltpu.VMEM((2, *flat), F32), pltpu.SemaphoreType.DMA((4,))],
        compiler_params=pltpu.CompilerParams(vmem_limit_bytes=4 * 1024 * 1024),
    )(*outs)
    return tuple(x.reshape(tokens, heads, depth) for x in outs)


def solution(mesh):
    spec, gain = P("seq", "head", None), P("head", None)
    return jax.shard_map(
        functools.partial(local, mesh.shape["seq"], mesh.shape["head"]),
        mesh=mesh,
        in_specs=(spec, spec, spec, gain, gain, spec),
        out_specs=(spec,) * 4,
        check_vma=False,
    )
```

```python
import functools

import jax
import jax.numpy as jnp
from jax import lax
from jax.experimental import pallas as pl
from jax.experimental.pallas import tpu as pltpu
from jax.sharding import PartitionSpec as P

MESH = pl.DeviceIdType.MESH
EPSILON = 1e-06
CHIPS_X = 4
F32, BF16 = jnp.float32, jnp.bfloat16

NN = ((1,), (0,))
NT = ((1,), (1,))
TN = ((0,), (0,))


def halves(x):
    high = x.astype(BF16)
    return high, (x - high.astype(F32)).astype(BF16)


def left_parts(x, axis):
    high, low = halves(x)
    return jnp.concatenate([high, low, high], axis=axis)


def right_parts(x, axis):
    high, low = halves(x)
    return jnp.concatenate([high, high, low], axis=axis)


def dot(left, right, form):
    return lax.dot_general(left, right, (form, ((), ())), preferred_element_type=F32)


def product(left, right, form):
    return dot(left_parts(left, form[0][0]), right_parts(right, form[1][0]), form)


def lane_sums(x):
    high, low = halves(x)
    rest = (x - high.astype(F32) - low.astype(F32)).astype(BF16)
    parts = jnp.concatenate([high, low, rest], axis=1)
    ones = jnp.ones((8, parts.shape[1]), BF16)
    return dot(ones, parts, NT)


def down_rows(line, i, tokens):
    return jnp.concatenate(
        [
            jnp.broadcast_to(line[2 * i + j : 2 * i + j + 1, :], (128, 128)).T
            for j in range(tokens // 128)
        ],
        axis=0,
    )


def kernel(
    n_seq, n_head, heads, tokens, depth,
    q_hbm, k_hbm, v_hbm, c_hbm, q_gain_hbm, k_gain_hbm,
    att_ref, gv_ref, push_ref, base_ref, mean_ref,
    raw, gains, unit, other, turned, split, first, second, mix, score, weight, scales,
    z_send, z_recv, z_cross, part_send, part_recv, line_scale, bare, peer_bare, peer_other,
    peer_split, peer_turned, states, chip_sum, gathered, prefixes, entering, passed, received,
    load_sem, z_sems, part_sems, push_sems, core_sems, scan_sems, give_sems,
):
    chips = n_seq // 2
    share = heads * depth // chips
    seq, head = lax.axis_index("seq"), lax.axis_index("head")
    chip, core = seq // 2, seq % 2
    width = float(heads * n_head * depth)

    loads = [
        pltpu.make_async_copy(src, raw.at[i], load_sem.at[i])
        for i, src in enumerate((q_hbm, k_hbm, v_hbm, c_hbm))
    ] + [
        pltpu.make_async_copy(src, gains.at[i], load_sem.at[4 + i])
        for i, src in enumerate((q_gain_hbm, k_gain_hbm))
    ]
    barrier = pltpu.get_barrier_semaphore()

    chips_x = min(CHIPS_X, chips)
    chips_y = chips // chips_x
    chip_y, chip_x = chip // chips_x, chip % chips_x
    steps = sorted(
        [(dy, dx) for dy in range(chips_y) for dx in range(chips_x) if dy or dx],
        key=lambda s: -(min(s[0], chips_y - s[0]) + min(s[1], chips_x - s[1])),
    )
    others = [
        lax.rem(chip_y + dy, chips_y) * chips_x + lax.rem(chip_x + dx, chips_x) for dy, dx in steps
    ]
    turns = sorted(range(1, n_head), key=lambda d: -min(d, n_head - d))
    heads_on = [lax.rem(head + d, n_head) for d in turns]
    peer_seq = 2 * chip + 1 - core
    partner = (peer_seq, head)
    greeted = [(0, partner)]
    for d, to in zip(turns, heads_on):
        greeted += [(min(d, n_head - d), (at, to)) for at in (seq, peer_seq)]
    for (dy, dx), to in zip(steps, others):
        hops = min(dy, chips_y - dy) + min(dx, chips_x - dx)
        greeted.append((hops, (2 * to + core, head)))
    for _, device in sorted(greeted, key=lambda pair: -pair[0]):
        pl.semaphore_signal(barrier, inc=1, device_id=device, device_id_type=MESH)
    for load in loads:
        load.start()

    def rows_of(h):
        return pl.ds(h, tokens, stride=heads)

    def share_sums(slot, of_query, of_key):
        send, recv = z_send.at[slot], z_recv.at[slot]
        for i, of_one in enumerate((of_query, of_key)):
            sums = lane_sums(of_one)
            for j in range(tokens // 128):
                send[pl.ds(2 * i + j, 1), :] = sums[0:1, 128 * j : 128 * (j + 1)]
        recv[head] = send[...]

    def share_copy(slot, to):
        return pltpu.make_async_remote_copy(
            src_ref=z_send.at[slot],
            dst_ref=z_recv.at[slot, head],
            send_sem=z_sems.at[2 * slot],
            recv_sem=z_sems.at[2 * slot + 1],
            device_id=(seq, to),
            device_id_type=MESH,
        )

    def send_shares(slot):
        for to in heads_on:
            share_copy(slot, to).start()

    def cross_copy(to):
        return pltpu.make_async_remote_copy(
            src_ref=z_send.at[0],
            dst_ref=z_cross.at[head],
            send_sem=z_sems.at[4],
            recv_sem=z_sems.at[5],
            device_id=(peer_seq, to),
            device_id_type=MESH,
        )

    def part_copy(kind, device):
        return pltpu.make_async_remote_copy(
            src_ref=part_send.at[kind],
            dst_ref=part_recv.at[kind, head],
            send_sem=part_sems.at[2 * kind],
            recv_sem=part_sems.at[2 * kind + 1],
            device_id=device,
            device_id_type=MESH,
        )

    def await_shares(slot):
        all_of = z_recv.at[slot, pl.ds(0, n_head - 1)]
        pltpu.make_async_copy(all_of, all_of, z_sems.at[2 * slot + 1]).wait()
        return jnp.sum(z_recv[slot], axis=0)

    loads[0].wait()
    loads[1].wait()
    query_squares = jnp.zeros((tokens, depth), F32)
    key_squares = jnp.zeros((tokens, depth), F32)
    for h in range(heads):
        q, k = raw[0, rows_of(h), :], raw[1, rows_of(h), :]
        query_squares += q * q
        key_squares += k * k
    share_sums(0, query_squares, key_squares)

    pl.semaphore_wait(barrier, len(greeted))
    for to in heads_on:
        share_copy(0, to).start()
        cross_copy(to).start()
    cross_copy(head).start()

    loads[2].wait()
    loads[3].wait()
    loads[4].wait()
    loads[5].wait()
    position = (seq * tokens + lax.broadcasted_iota(jnp.int32, (tokens, depth), 0)).astype(F32)
    weight[...] = lax.rsqrt(float(depth) * (position + 1.0))
    for h in range(heads):
        other[0, h] = raw[3, rows_of(h), :] * weight[...]
        other[1, h] = raw[2, rows_of(h), :]
    for i in range(2):
        for h in range(heads):
            bare[i, h] = raw[i, rows_of(h), :] * gains[i, pl.ds(h, 1), :]

    pushes = [
        pltpu.make_async_remote_copy(
            src_ref=src,
            dst_ref=dst,
            send_sem=push_sems.at[2 * i],
            recv_sem=push_sems.at[2 * i + 1],
            device_id=partner,
            device_id_type=MESH,
        )
        for i, (src, dst) in enumerate(
            ((other, peer_other), (bare, peer_bare))
        )
    ]
    for push in pushes:
        push.start()

    def turning(h, _):
        for i in range(2):
            turned[i, h] = left_parts(other[i, h].T, 1)
            split[i, h] = left_parts(other[i, h], 1)
        return 0

    lax.fori_loop(0, heads, turning, 0)

    rows = lax.broadcasted_iota(jnp.int32, (tokens, tokens), 0)
    columns = lax.broadcasted_iota(jnp.int32, (tokens, tokens), 1)
    causal = rows >= columns

    def mixing(h, _):
        mix[h] = jnp.where(causal, product(other[0, h], other[1, h], NT), 0.0)
        return 0

    lax.fori_loop(0, heads, mixing, 0)

    for push in pushes:
        push.wait_recv()

    def turning_peer(h, _):
        peer_turned[h] = left_parts(peer_other[1 - core, h].T, 1)
        return 0

    lax.fori_loop(0, heads, turning_peer, 0)

    def scale_of(total):
        return lax.rsqrt(total / width + EPSILON)

    def at_head(h):
        return pl.ds(h * depth, depth)

    pairs = tokens // 128

    def of_kind(lines, first_kind):
        return jnp.where(first_kind, lines[:pairs, :], lines[pairs:, :])

    scale = scale_of(await_shares(0))
    pltpu.make_async_copy(z_cross, z_cross, z_sems.at[5]).wait()
    peer_scale = scale_of(jnp.sum(z_cross[...], axis=0))
    line_scale[...] = scale
    down = down_rows(of_kind(scale, core == 1), 0, tokens)
    peer_down = down_rows(of_kind(peer_scale, core == 1), 0, tokens)
    scales[1 - core] = down
    def scan_rows(c):
        return pl.ds(pl.multiple_of(c * share, share), share)

    def scan_copy(src, dst, send_sem, recv_sem, to):
        return pltpu.make_async_remote_copy(
            src_ref=src,
            dst_ref=dst,
            send_sem=send_sem,
            recv_sem=recv_sem,
            device_id=(2 * to + core, head),
            device_id_type=MESH,
        )

    per_head = chips // heads
    block = chip // per_head

    for far in sorted(range(heads), key=lambda k: -min(k, heads - k)):
        h = lax.rem(block + far, heads)
        normed = right_parts(bare[1 - core, h] * down, 0)
        peer_normed = right_parts(peer_bare[1 - core, h] * peer_down, 0)
        chip_sum[pl.ds(pl.multiple_of(h * depth, depth), depth), :] = dot(
            jnp.concatenate([turned[1 - core, h], peer_turned[h]], axis=1),
            jnp.concatenate([normed, peer_normed], axis=0),
            NN,
        )
        spots = range(per_head) if far else range(1, per_head)
        for j in sorted(spots, key=lambda j: -min(j % CHIPS_X, CHIPS_X - j % CHIPS_X)):
            to = h * per_head + lax.rem(chip + j, per_head)
            scan_copy(
                chip_sum.at[scan_rows(to)], gathered.at[chip], scan_sems.at[0], scan_sems.at[1], to
            ).start()

    def to_partner(src, dst, h):
        return pltpu.make_async_remote_copy(
            src_ref=src.at[at_head(h)],
            dst_ref=dst.at[at_head(h)],
            send_sem=core_sems.at[0, h],
            recv_sem=core_sems.at[1, h],
            device_id=partner,
            device_id_type=MESH,
        )

    gathered[chip] = chip_sum[scan_rows(chip), :]

    def scoring(h, _):
        for i in range(2):
            unit[i, h] = bare[i, h] * scales[i]
        states[pl.ds(pl.multiple_of(h * depth, depth), depth), :] = dot(
            turned[1 - core, h], right_parts(unit[1 - core, h], 0), NN
        )
        score[h] = jnp.where(causal, product(unit[0, h], unit[1, h], NT), 0.0)
        peer_split[h] = left_parts(peer_other[core, h], 1)
        return 0

    scales[core] = down_rows(of_kind(scale, core == 0), 0, tokens)
    lax.fori_loop(0, heads, scoring, 0)
    all_others = gathered.at[pl.ds(0, chips - 1)]
    pltpu.make_async_copy(all_others, all_others, scan_sems.at[1]).wait()

    running = jnp.zeros((share, depth), F32)
    for i in range(chips):
        c = i + core * (chips - 1 - 2 * i)
        prefixes[c] = running
        running = running + gathered[c]

    for to in others:
        scan_copy(
            prefixes.at[to],
            entering.at[scan_rows(chip)],
            give_sems.at[heads],
            give_sems.at[block],
            to,
        ).start()
    pltpu.make_async_copy(
        prefixes.at[chip], entering.at[scan_rows(chip)], give_sems.at[block]
    ).start()

    def inside(h, _):
        first[0, h] = product(score[h], other[1, h], NN)
        second[0, h] = product(mix[h], unit[1, h], NN)
        first[1, h] = product(score[h], other[0, h], TN)
        second[1, h] = product(mix[h], unit[0, h], TN)
        return 0

    lax.fori_loop(0, heads, inside, 0)
    inner = [jnp.zeros((tokens, depth), F32) for _ in range(2)]
    for h in range(heads):
        for i in range(2):
            inner[i] += unit[i, h] * second[i, h]
    share_sums(1, *inner)
    send_shares(1)
    def apply_first(which, state):
        def body(h, _):
            held = state[pl.ds(pl.multiple_of(h * depth, depth), depth), :]
            first[which, h] += product(unit[which, h], held, NT)
            return 0

        lax.fori_loop(0, heads, body, 0)

    own_inner = jnp.zeros((tokens, depth), F32)
    peer_inner = jnp.zeros((tokens, depth), F32)
    for far in sorted(range(heads), key=lambda k: -min(k, heads - k)):
        h = lax.rem(block + far, heads)
        here = pl.ds(pl.multiple_of(h * depth, depth), depth)
        one_head = gathered.at[pl.ds(0, per_head)]
        pltpu.make_async_copy(one_head, one_head, give_sems.at[h]).wait()
        held = entering[here, :]
        next_held = held + states[here, :]
        passed[here, :] = next_held
        pushed = dot(split[core, h], right_parts(held, 0), NN)
        second[core, h] += pushed
        own_inner += unit[core, h] * pushed
        peer_inner += peer_bare[core, h] * dot(peer_split[h], right_parts(next_held, 0), NN)
    hands = [to_partner(passed, received, h) for h in range(heads)]
    for kind, of_one in enumerate((own_inner, peer_inner)):
        sums = lane_sums(of_one)
        for j in range(tokens // 128):
            part_send[kind, pl.ds(j, 1), :] = sums[0:1, 128 * j : 128 * (j + 1)]
    for to in heads_on:
        part_copy(0, (seq, to)).start()
        part_copy(1, (peer_seq, to)).start()
    part_copy(1, partner).start()
    part_recv[0, head] = part_send[0]
    for hand in hands:
        hand.start()

    for h in range(heads):
        hands[h].wait_recv()
        second[1 - core, h] += dot(
            split[1 - core, h], right_parts(received[at_head(h), :], 0), NN
        )
    apply_first(core, entering)
    apply_first(1 - core, received)
    for h in range(heads):
        att_ref[rows_of(h), :] = first[0, h] * weight[...]
        gv_ref[rows_of(h), :] = first[1, h]
    for i in range(2):
        for h in range(heads):
            push_ref[i, h] = second[i, h] * gains[i, pl.ds(h, 1), :] * scales[i]
            base_ref[i, h] = raw[i, rows_of(h), :] * (scales[i] * scales[i])
    inside_total = await_shares(1)
    others_here = part_recv.at[0, pl.ds(0, n_head - 1)]
    pltpu.make_async_copy(others_here, others_here, part_sems.at[1]).wait()
    pltpu.make_async_copy(part_recv.at[1], part_recv.at[1], part_sems.at[3]).wait()
    own_part = jnp.sum(part_recv[0], axis=0)
    peer_part = jnp.sum(part_recv[1], axis=0)
    for i in range(2):
        rows = slice(pairs * i, pairs * (i + 1))
        part = jnp.where(core == i, own_part, peer_part * line_scale[rows, :])
        mean_ref[rows, :] = (inside_total[rows, :] + part) / width

    for h in range(heads):
        hands[h].wait_send()
    for push in pushes:
        push.wait_send()
    pltpu.make_async_copy(others_here, others_here, part_sems.at[0]).wait()
    pltpu.make_async_copy(part_recv.at[1], part_recv.at[1], part_sems.at[2]).wait()
    pltpu.make_async_copy(z_cross, z_cross, z_sems.at[4]).wait()
    for slot in range(2):
        all_of = z_recv.at[slot, pl.ds(0, n_head - 1)]
        pltpu.make_async_copy(all_of, all_of, z_sems.at[2 * slot]).wait()
    for sem in (scan_sems.at[0], give_sems.at[heads]):
        pltpu.make_async_copy(all_others, all_others, sem).wait()


def leave(
    heads, tokens, att_ref, gv_ref, push_ref, base_ref, mean_ref,
    att_out, gq_out, gk_out, gv_out, staged, sems,
):
    copies = [
        pltpu.make_async_copy(src, dst, sems.at[i])
        for i, (src, dst) in enumerate(
            ((att_ref, att_out), (gv_ref, gv_out), (staged.at[0], gq_out), (staged.at[1], gk_out))
        )
    ]
    copies[0].start()
    copies[1].start()
    mean = mean_ref[...]
    for i in range(2):
        along = down_rows(mean, i, tokens)
        for h in range(heads):
            rows = pl.ds(h, tokens, stride=heads)
            staged[i, rows, :] = push_ref[i, h] - base_ref[i, h] * along
        copies[2 + i].start()
    for copy in copies:
        copy.wait()


def kept(x):
    return pltpu.with_memory_space_constraint(x, pltpu.HBM)


def local(n_seq, n_head, query_raw, key_raw, value_raw, query_gain, key_gain, cotangent):
    tokens, heads, depth = query_raw.shape
    chips = n_seq // 2
    flat = (tokens * heads, depth)
    both = (2, heads, tokens, depth)
    states = (heads * depth, depth)
    per_owner = (chips, heads * depth // chips, depth)
    hbm = pl.BlockSpec(memory_space=pltpu.HBM)
    vmem = pl.BlockSpec(memory_space=pltpu.VMEM)
    outs = pl.pallas_call(
        functools.partial(kernel, n_seq, n_head, heads, tokens, depth),
        out_shape=[
            jax.ShapeDtypeStruct(shape, F32)
            for shape in (flat, flat, both, both, (2 * tokens // 128, 128))
        ],
        in_specs=[hbm] * 6,
        out_specs=[vmem] * 5,
        scratch_shapes=[
            pltpu.VMEM((4, *flat), F32),
            pltpu.VMEM((2, heads, depth), F32),
            pltpu.VMEM(both, F32),
            pltpu.VMEM(both, F32),
            pltpu.VMEM((2, heads, depth, 3 * tokens), BF16),
            pltpu.VMEM((2, heads, tokens, 3 * depth), BF16),
            pltpu.VMEM(both, F32),
            pltpu.VMEM(both, F32),
            pltpu.VMEM((heads, tokens, tokens), F32),
            pltpu.VMEM((heads, tokens, tokens), F32),
            pltpu.VMEM((tokens, depth), F32),
            pltpu.VMEM((2, tokens, depth), F32),
            pltpu.VMEM((2, 2 * tokens // 128, 128), F32),
            pltpu.VMEM((2, n_head, 2 * tokens // 128, 128), F32),
            pltpu.VMEM((n_head, 2 * tokens // 128, 128), F32),
            pltpu.VMEM((2, tokens // 128, 128), F32),
            pltpu.VMEM((2, n_head, tokens // 128, 128), F32),
            pltpu.VMEM((2 * tokens // 128, 128), F32),
            pltpu.VMEM(both, F32),
            pltpu.VMEM(both, F32),
            pltpu.VMEM(both, F32),
            pltpu.VMEM((heads, tokens, 3 * depth), BF16),
            pltpu.VMEM((heads, depth, 3 * tokens), BF16),
            pltpu.VMEM(states, F32),
            pltpu.VMEM(states, F32),
            pltpu.VMEM(per_owner, F32),
            pltpu.VMEM(per_owner, F32),
            pltpu.VMEM(states, F32),
            pltpu.VMEM(states, F32),
            pltpu.VMEM(states, F32),
            pltpu.SemaphoreType.DMA((6,)),
            pltpu.SemaphoreType.DMA((6,)),
            pltpu.SemaphoreType.DMA((4,)),
            pltpu.SemaphoreType.DMA((4,)),
            pltpu.SemaphoreType.DMA((2, heads)),
            pltpu.SemaphoreType.DMA((2,)),
            pltpu.SemaphoreType.DMA((heads + 1,)),
        ],
        compiler_params=pltpu.CompilerParams(
            collective_id=0, has_side_effects=True, vmem_limit_bytes=48 * 1024 * 1024
        ),
    )(
        *(kept(x.reshape(flat)) for x in (query_raw, key_raw, value_raw, cotangent)),
        kept(query_gain),
        kept(key_gain),
    )
    outs = pl.pallas_call(
        functools.partial(leave, heads, tokens),
        out_shape=[jax.ShapeDtypeStruct(flat, F32)] * 4,
        in_specs=[vmem] * 5,
        out_specs=[hbm] * 4,
        scratch_shapes=[pltpu.VMEM((2, *flat), F32), pltpu.SemaphoreType.DMA((4,))],
        compiler_params=pltpu.CompilerParams(vmem_limit_bytes=4 * 1024 * 1024),
    )(*outs)
    return tuple(x.reshape(tokens, heads, depth) for x in outs)


def solution(mesh):
    spec, gain = P("seq", "head", None), P("head", None)
    return jax.shard_map(
        functools.partial(local, mesh.shape["seq"], mesh.shape["head"]),
        mesh=mesh,
        in_specs=(spec, spec, spec, gain, gain, spec),
        out_specs=(spec,) * 4,
        check_vma=False,
    )
```
